32 devices in a mesh: row: 8 (over y, x, core), col: 4 (over z).
Axes of the slice: x: 2, y: 2, z: 4, core: 2. Of those that a mesh axis runs over, the one named last changes fastest.
Arguments:
- tensor: float32 [128, 128, 768], P('row', 'col'), may hold values from -6 to 6
- start_one: float32 [128, 64], P('row'), may hold values from -0.5 to 0.5
- start_two: float32 [128, 64], P('col'), may hold values from -0.5 to 0.5
- start_three: float32 [768, 64], replicated, may hold values from -0.21875 to 0.21875
Outputs:
- factor_one: float32 [128, 64], replicated
- factor_two: float32 [128, 64], replicated
- factor_three: float32 [768, 64], replicated
- core: float32 [64, 64, 64], P(None, 'row', 'col')
The draws below stay inside these ranges and needn't reach their ends.
All inputs are finite; a program needn't handle non-finite values.
Results may differ from the reference program's by a relative error of at most 0.0003.
Values sent between devices are 32-bit elements; how exact they have to be, the bound alone decides.
A program may use at most 64 MiB of HBM per device.

```python
import math
import jax
import jax.numpy as jnp
from jax import lax

N3 = 768
RANK = 64
STEPS = 4
N1 = 128
N2 = 128


def levels(key, extent, cuts, least, top_value):
    def one(position, parts):
        steps = jax.random.uniform(jax.random.fold_in(jax.random.fold_in(key, 6), position), (parts,), jnp.float32, least / len(cuts), top_value / len(cuts))
        return jnp.repeat(jnp.exp(steps), extent[position] // parts).reshape((-1,) + (1,) * (len(extent) - position - 1))

    gain = one(*cuts[0])
    for cut in cuts[1:]:
        gain = gain * one(*cut)
    return gain


def centred(own_key, extent, scale, reach, shards=(), held_as=jnp.bfloat16):
    gain = levels(own_key, extent, shards, -0.22, 0.18) if shards else 1.0
    array = jax.random.normal(own_key, extent, jnp.float32) * scale * gain
    return jnp.minimum(jnp.maximum(array, -reach), reach).astype(held_as)


def setup_inputs(seed: int = 0) -> dict:
    seeds = jax.random.split(jax.random.key(seed), 5)
    return {
        "tensor": centred(seeds[0], (N1, N2, N3), 1.0, 6.0, ((0, 8), (1, 4)), jnp.float32),
        "start_one": centred(seeds[1], (N1, RANK), N1 ** -0.5, 0.5, ((0, 8),), jnp.float32),
        "start_two": centred(seeds[2], (N2, RANK), N2 ** -0.5, 0.5, ((0, 4),), jnp.float32),
        "start_three": centred(seeds[3], (N3, RANK), N3 ** -0.5, 0.21875, (), jnp.float32),
    }


HIGHEST = lax.Precision.HIGHEST

def orthonormal(matrix):
    inner = jnp.dot(matrix.T.astype(jnp.float32), matrix.astype(jnp.float32), precision=HIGHEST, preferred_element_type=jnp.float32)
    lower = jnp.linalg.cholesky(inner)
    return jax.scipy.linalg.solve_triangular(lower, matrix.T, lower=True).T

def iterate(gram, start):
    basis = start
    for iteration in range(STEPS):
        basis = orthonormal(jnp.dot(gram.astype(jnp.float32), basis.astype(jnp.float32), precision=HIGHEST, preferred_element_type=jnp.float32))
    return basis

def self_gram(slab):
    return jnp.dot(slab.astype(jnp.float32), slab.T.astype(jnp.float32), precision=HIGHEST, preferred_element_type=jnp.float32)

def reference(tensor, start_one, start_two, start_three):
    contracted = jnp.einsum('ijk,kc->ijc', tensor, start_three, precision=HIGHEST)
    slab_one = jnp.einsum('ijc,jb->ibc', contracted, start_two, precision=HIGHEST).reshape(N1, RANK * RANK)
    basis_one = iterate(self_gram(slab_one), start_one)
    slab_two = jnp.einsum('ijc,ia->jac', contracted, basis_one, precision=HIGHEST).reshape(N2, RANK * RANK)
    basis_two = iterate(self_gram(slab_two), start_two)
    partial_three = jnp.einsum('ijk,ia->ajk', tensor, basis_one, precision=HIGHEST)
    slab_three = jnp.einsum('ajk,jb->kab', partial_three, basis_two, precision=HIGHEST).reshape(N3, RANK * RANK)
    basis_three = iterate(self_gram(slab_three), start_three)
    core = jnp.dot(basis_three.T.astype(jnp.float32), slab_three.astype(jnp.float32), precision=HIGHEST, preferred_element_type=jnp.float32).reshape(RANK, RANK, RANK)
    factor_one = basis_one * math.sqrt(N1)
    factor_two = basis_two * math.sqrt(N2)
    factor_three = basis_three * math.sqrt(N3)
    return (factor_one, factor_two, factor_three, core)
```

```python
import functools
import math
import types

import jax
import jax.numpy as jnp
from jax import lax
from jax.experimental import pallas as pl
from jax.experimental.pallas import tpu as pltpu
from jax.sharding import PartitionSpec as P

STEPS = 4


HIGHEST = lax.Precision.HIGHEST
MESH = pl.DeviceIdType.MESH
SUBLANES = 8
LANES = 128


def product(left, right):
    return jnp.dot(left, right, precision=HIGHEST, preferred_element_type=jnp.float32)


def left_product(left, right):
    return lax.dot_general(
        left, right, (((0,), (0,)), ((), ())), precision=HIGHEST, preferred_element_type=jnp.float32
    )


def right_product(left, right):
    return lax.dot_general(
        left, right, (((1,), (1,)), ((), ())), precision=HIGHEST, preferred_element_type=jnp.float32
    )


def cross_product(left, right):
    return lax.dot_general(
        left, right, (((0,), (1,)), ((), ())), precision=HIGHEST, preferred_element_type=jnp.float32
    )


def orthonormal(matrix, inner):
    lower = jnp.linalg.cholesky(inner)
    return jax.scipy.linalg.solve_triangular(lower, matrix.T, lower=True).T


def settle(gram_whole, basis):
    for iteration in range(STEPS):
        image = product(gram_whole, basis)
        basis = orthonormal(image, left_product(image, image))
    return basis


def general(tensor, start_one, start_two, start_three):
    rows_one, rows_two, depth = tensor.shape
    rank = start_three.shape[1]
    flat = tensor.reshape(rows_one * rows_two, depth)
    contracted = cross_product(start_three, flat).reshape(rank, rows_one, rows_two)
    part_one = jnp.einsum("cij,jb->ibc", contracted, start_two, precision=HIGHEST).reshape(
        rows_one, rank * rank
    )
    slab_one = lax.psum_scatter(part_one, "col", scatter_dimension=1, tiled=True)
    slab_rows_one = lax.all_gather(slab_one, "row", axis=0, tiled=True)
    gram_one = lax.psum(right_product(slab_rows_one, slab_rows_one), "col")
    basis_one = settle(gram_one, lax.all_gather(start_one, "row", axis=0, tiled=True))
    own_one = lax.dynamic_slice_in_dim(basis_one, lax.axis_index("row") * rows_one, rows_one, 0)
    part_two = jnp.einsum("cij,ia->jac", contracted, own_one, precision=HIGHEST).reshape(
        rows_two, rank * rank
    )
    slab_two = lax.psum_scatter(part_two, "row", scatter_dimension=1, tiled=True)
    slab_rows_two = lax.all_gather(slab_two, "col", axis=0, tiled=True)
    gram_two = lax.psum(right_product(slab_rows_two, slab_rows_two), "row")
    basis_two = settle(gram_two, lax.all_gather(start_two, "col", axis=0, tiled=True))
    own_two = lax.dynamic_slice_in_dim(basis_two, lax.axis_index("col") * rows_two, rows_two, 0)
    received = lax.all_to_all(tensor, "row", split_axis=2, concat_axis=0, tiled=True)
    count, items, cells = received.shape
    merged = left_product(basis_one, received.reshape(count, items * cells))
    mixed = merged.reshape(rank, items, cells)
    part_three = jnp.einsum("ajk,jb->kba", mixed, own_two, precision=HIGHEST)
    cells_here = part_three.shape[0]
    slab_three = lax.psum_scatter(
        part_three.reshape(cells_here, rank * rank), "col", scatter_dimension=1, tiled=True
    )
    gram_part_three = right_product(slab_three, lax.all_gather(slab_three, "row", axis=0, tiled=True))
    gram_three = lax.psum(gram_part_three, "col")
    basis_three = start_three
    own_three = start_three
    for iteration in range(STEPS):
        image = product(gram_three, basis_three)
        inner = lax.psum(left_product(image, image), "row")
        own_three = orthonormal(image, inner)
        basis_three = lax.all_gather(own_three, "row", axis=0, tiled=True)
    core_part = left_product(own_three, slab_three)
    core_part = core_part.reshape(rank, core_part.shape[1] // rank, rank)
    core = lax.psum_scatter(core_part, "row", scatter_dimension=2, tiled=True).transpose(0, 2, 1)
    factor_one = basis_one * math.sqrt(basis_one.shape[0])
    factor_two = basis_two * math.sqrt(basis_two.shape[0])
    factor_three = basis_three * math.sqrt(basis_three.shape[0])
    return (factor_one, factor_two, factor_three, core)


def inverse_factor(inner):
    n = inner.shape[0]
    groups = n // SUBLANES
    eye = (
        lax.broadcasted_iota(jnp.int32, (n, n), 0) == lax.broadcasted_iota(jnp.int32, (n, n), 1)
    ).astype(jnp.float32)
    whole = jnp.concatenate([inner, eye], axis=1)
    width = whole.shape[1]
    rows = [whole[g * SUBLANES : (g + 1) * SUBLANES] for g in range(groups)]
    sub = lax.broadcasted_iota(jnp.int32, (SUBLANES, width), 0)
    pivots = [None] * n
    shape = (SUBLANES, width)
    for base in range(groups):
        columns = [
            [jnp.broadcast_to(rows[g][:, k : k + 1], shape) for g in range(base, groups)]
            for k in range(base * SUBLANES, (base + 1) * SUBLANES)
        ]
        for t in range(SUBLANES):
            pivot = jnp.broadcast_to(columns[t][0][t : t + 1, :], shape)
            scale = 1.0 / pivot
            pivots[base * SUBLANES + t] = pivot
            row = jnp.broadcast_to(rows[base][t : t + 1, :], shape)
            heads = [
                jnp.broadcast_to(columns[s][0][t : t + 1, :], shape) for s in range(t + 1, SUBLANES)
            ]
            for g in range(base, groups):
                factor = columns[t][g - base] * scale
                if g == base:
                    factor = jnp.where(sub > t, factor, 0.0)
                rows[g] = rows[g] - factor * row
                for s in range(t + 1, SUBLANES):
                    columns[s][g - base] = columns[s][g - base] - factor * heads[s - t - 1]
    out = []
    for g in range(groups):
        held = pivots[g * SUBLANES]
        for t in range(1, SUBLANES):
            held = jnp.where(sub == t, pivots[g * SUBLANES + t], held)
        out.append(rows[g] * lax.rsqrt(held))
    return jnp.concatenate(out, axis=0)[:, n:]


def lane_groups(width):
    return lax.div(lax.broadcasted_iota(jnp.int32, (1, LANES), 1), width)


def shifted(value, amount):
    amount = amount % LANES
    return value if amount == 0 else pltpu.roll(value, amount, 1)


def settle_turned(gram_ref, basis_ref):
    def one(_, carry):
        image = product(basis_ref[...], gram_ref[...])
        basis_ref[...] = product(inverse_factor(right_product(image, image)), image)
        return carry

    lax.fori_loop(0, STEPS, one, 0)


def aligned(start, count, multiple=SUBLANES):
    return pl.ds(pl.multiple_of(start, multiple), count)


def remote(source, target, send, recv, row, col):
    return pltpu.make_async_remote_copy(
        src_ref=source, dst_ref=target, send_sem=send, recv_sem=recv, device_id=(row, col), device_id_type=MESH
    )


def start_all(made):
    for copy in made:
        copy.start()
    return made


def greet_all(n_row, n_col):
    n = n_row * n_col
    me = lax.axis_index("row") * n_col + lax.axis_index("col")
    barrier = pltpu.get_barrier_semaphore()

    def one(d, carry):
        peer = lax.rem(me + d, n)
        pl.semaphore_signal(
            barrier, inc=1, device_id=(peer // n_col, lax.rem(peer, n_col)), device_id_type=MESH
        )
        return carry

    lax.fori_loop(1, n, one, 0)
    return barrier


def chain_scratch(n_row, n_col, rows_one, rows_two, depth, rank):
    n, chips, plane = n_row * n_col, n_row * n_col // 2, n_row // 2
    half, blocks, chunk, n_one, n_two = depth // 2, rank // chips, rank // plane, LANES, LANES
    share = rank // n

    def buffer(*shape):
        return pltpu.VMEM(shape, jnp.float32)

    def dma(*shape):
        return pltpu.SemaphoreType.DMA(shape)

    return dict(
        parted=buffer(n * SUBLANES, LANES),
        held=buffer(n * SUBLANES, LANES),
        faces=buffer(share * n_one, n_two),
        turned=buffer(share, n_two, n_one),
        all_one=buffer(n_one, rank),
        all_two=buffer(n_two, rank),
        gram_part=buffer(2, LANES, LANES),
        gram_parts=buffer(2, n_row, LANES // n_row, LANES),
        gram_planes=buffer(2, n_col, LANES // n_row, LANES),
        gram_sum=buffer(2, LANES, LANES),
        basis_one=buffer(rank, n_one),
        basis_two=buffer(rank, n_two),
        block=buffer(half // LANES, n_one, SUBLANES, LANES),
        mixed=buffer(half // LANES, rank, SUBLANES, LANES),
        joined=buffer(half // LANES, blocks, n_two, LANES),
        slab=buffer(blocks * rank, half),
        image=buffer(STEPS + 1, rank, half),
        cross_own=buffer(STEPS, rank, blocks * rank),
        cross_pair=buffer(STEPS, rank, blocks * rank),
        inner_own=buffer(STEPS + 1, rank, rank),
        inner_pair=buffer(STEPS + 1, rank, rank),
        image_part=buffer(STEPS, rank, half),
        image_parts=buffer(STEPS, plane, chunk, half),
        image_planes=buffer(STEPS, n_col, chunk, half),
        last=buffer(rank, half),
        core_own=buffer(blocks * rank, rank),
        core_pair=buffer(blocks * rank, rank),
        core_sum=buffer(blocks, rank, rank),
        core_all=buffer(n_col * blocks, rank // n_col, rank),
        s_held=dma(n), r_held=dma(n),
        s_one=dma(n_row), r_one=dma(n_row),
        s_two=dma(n_col), r_two=dma(n_col),
        s_block=dma(half // LANES, n_row), r_block=dma(half // LANES, n_row),
        own=dma(half // LANES),
        s_gram_row=dma(2, n_row), r_gram_row=dma(2, n_row),
        s_gram_col=dma(2, n_col), r_gram_col=dma(2, n_col),
        s_gram_all=dma(2, n_row), r_gram_all=dma(2, n_row),
        s_mixed=dma(chips), r_mixed=dma(chips),
        s_cross=dma(STEPS), r_cross=dma(STEPS),
        s_inner=dma(STEPS + 1), r_inner=dma(STEPS + 1),
        s_image_row=dma(STEPS, plane), r_image_row=dma(STEPS, plane),
        s_image_col=dma(STEPS, n_col), r_image_col=dma(STEPS, n_col),
        s_image_all=dma(STEPS, plane), r_image_all=dma(STEPS, plane),
        s_last=dma(2), r_last=dma(2),
        s_core=dma(n_col), r_core=dma(n_col),
    )


def chain_kernel(n_row, n_col, names, t_ref, v_ref, one_ref, two_ref, f1_ref, f2_ref, last_ref, linv_ref, piece_ref, *refs):
    g = types.SimpleNamespace(**dict(zip(names, refs)))
    row, col = lax.axis_index("row"), lax.axis_index("col")
    n, plane, chips = n_row * n_col, n_row // 2, n_row * n_col // 2
    me, chip, core = row * n_col + col, row // 2, lax.rem(row, 2)
    other = row + 1 - 2 * core
    rows_one, rows_two, depth = t_ref.shape
    rank, half = v_ref.shape[0], depth // 2
    share, tiles = rank // n, rows_one * rows_two // LANES
    n_one = n_two = LANES

    def row_peer(d):
        return lax.rem(row + d, n_row)

    def col_peer(d):
        return lax.rem(col + d, n_col)

    def plane_peer(d):
        return lax.rem(chip + d, plane)

    barrier = greet_all(n_row, n_col)
    contracted = right_product(v_ref[...], t_ref[...].reshape(rows_one * rows_two, depth))
    for tile in range(tiles):
        g.parted[pl.ds(tile, rank, stride=tiles), :] = contracted[:, tile * LANES : (tile + 1) * LANES]
    pl.semaphore_wait(barrier, n - 1)
    place = col * n_row + row

    def held_copy(d):
        peer = lax.rem(me + d, n)
        return remote(
            g.parted.at[aligned(peer * SUBLANES, SUBLANES), :],
            g.held.at[aligned(place * SUBLANES, SUBLANES), :],
            g.s_held.at[d], g.r_held.at[d], peer // n_col, lax.rem(peer, n_col),
        )

    def held_start(d, carry):
        held_copy(d).start()
        return carry

    def held_wait(d, carry):
        held_copy(d).wait()
        return carry

    lax.fori_loop(1, n, held_start, 0)
    own_one, own_two = aligned(row * rows_one, rows_one), aligned(col * rows_two, rows_two)
    starts = start_all(
        [remote(two_ref, g.all_two.at[own_two, :], g.s_two.at[d], g.r_two.at[d], row, col_peer(d)) for d in range(1, n_col)]
        + [remote(one_ref, g.all_one.at[own_one, :], g.s_one.at[d], g.r_one.at[d], row_peer(d), col) for d in range(1, n_row)]
    )

    portions = half // LANES

    def block_source(which, peer):
        return t_ref.at[
            :,
            aligned(peer // 2 * SUBLANES, SUBLANES),
            aligned(lax.rem(peer, 2) * half + which * LANES, LANES, LANES),
        ]

    def block_target(which):
        return g.block.at[which, pl.ds(row * rows_one, rows_one)]

    def block_copies(which):
        return [
            remote(
                block_source(which, row_peer(d)), block_target(which),
                g.s_block.at[which, d], g.r_block.at[which, d], row_peer(d), col,
            )
            for d in range(1, n_row)
        ]

    bulk = start_all(block_copies(0))
    kept = start_all(
        [pltpu.make_async_copy(block_source(w, row), block_target(w), g.own.at[w]) for w in range(portions)]
    )
    g.held[aligned(place * SUBLANES, SUBLANES), :] = g.parted[aligned(me * SUBLANES, SUBLANES), :]
    g.all_one[own_one, :] = one_ref[...]
    g.all_two[own_two, :] = two_ref[...]
    g.image[0] = v_ref[:, aligned(core * half, half, LANES)]
    linv_ref[...] = unit(rank)
    for copy in starts:
        copy.wait()
    lax.fori_loop(1, n, held_wait, 0)
    group = lane_groups(rows_two)
    for c in range(share):
        for tile in range(tiles):
            blocks = [
                g.held[pl.ds(q * n_row * SUBLANES + c * tiles + tile, n_row, stride=SUBLANES), :] for q in range(n_col)
            ]
            for s in range(n_col):
                line = shifted(blocks[0], -s * rows_two)
                for q in range(1, n_col):
                    line = jnp.where(group == q, shifted(blocks[q], (q - s) * rows_two), line)
                g.faces[pl.ds(c * n_one + tile * n_col + s, n_row, stride=rows_one), :] = line

    count = LANES // n_row
    own_rows = aligned(row * count, count)

    def gram_first(w):
        return start_all(
            [
                remote(
                    g.gram_part.at[w, aligned(row_peer(d) * count, count), :], g.gram_parts.at[w, d],
                    g.s_gram_row.at[w, d], g.r_gram_row.at[w, d], row_peer(d), col,
                )
                for d in range(1, n_row)
            ]
        )

    def gram_second(w, first):
        total = g.gram_part[w, own_rows, :]
        for d in range(1, n_row):
            first[d - 1].wait_recv()
            total = total + g.gram_parts[w, d]
        g.gram_planes[w, col] = total
        return start_all(
            [
                remote(
                    g.gram_planes.at[w, col], g.gram_planes.at[w, col],
                    g.s_gram_col.at[w, d], g.r_gram_col.at[w, d], row, col_peer(d),
                )
                for d in range(1, n_col)
            ]
        )

    def gram_third(w, second):
        for copy in second:
            copy.wait_recv()
        total = g.gram_planes[w, 0]
        for q in range(1, n_col):
            total = total + g.gram_planes[w, q]
        g.gram_sum[w, own_rows, :] = total
        return start_all(
            [
                remote(
                    g.gram_sum.at[w, own_rows, :], g.gram_sum.at[w, own_rows, :],
                    g.s_gram_all.at[w, d], g.r_gram_all.at[w, d], row_peer(d), col,
                )
                for d in range(1, n_row)
            ]
        )

    def gram_end(first, second, third):
        for copy in third:
            copy.wait_recv()
        for copy in first + second + third:
            copy.wait_send()

    def self_gram(slabs):
        total = right_product(slabs[0], slabs[0])
        for slab in slabs[1:]:
            total = total + right_product(slab, slab)
        return total

    g.gram_part[0] = self_gram(
        [product(g.faces[c * n_one : (c + 1) * n_one, :], g.all_two[...]) for c in range(share)]
    )
    first = gram_first(0)
    for c in range(share):
        g.turned[c] = g.faces[c * n_one : (c + 1) * n_one, :].T
    g.basis_one[...] = g.all_one[...].T
    g.basis_two[...] = g.all_two[...].T
    second = gram_second(0, first)
    third = gram_third(0, second)
    gram_end(first, second, third)
    for which in range(1, portions):
        bulk = bulk + start_all(block_copies(which))
    settle_turned(g.gram_sum.at[0], g.basis_one)
    basis_one = g.basis_one[...]

    g.gram_part[1] = self_gram([right_product(g.turned[c], basis_one) for c in range(share)])
    first = gram_first(1)
    f1_ref[...] = basis_one * math.sqrt(n_one)
    for copy in bulk:
        copy.wait()
    for copy in kept:
        copy.wait()
    flat_block = g.block.reshape(portions * n_one * SUBLANES, LANES)
    flat_mixed = g.mixed.reshape(portions * rank * SUBLANES, LANES)
    for s in range(SUBLANES):
        face = [flat_block[pl.ds(w * n_one * SUBLANES + s, n_one, stride=SUBLANES), :] for w in range(portions)]
        face = product(basis_one, jnp.concatenate(face, axis=1))
        for w in range(portions):
            flat_mixed[pl.ds(w * rank * SUBLANES + s, rank, stride=SUBLANES), :] = face[:, w * LANES : (w + 1) * LANES]
    second = gram_second(1, first)
    third = gram_third(1, second)
    gram_end(first, second, third)

    pieces = rank // chips
    place = chip * n_col + col
    lines = aligned(col * rows_two + chip * SUBLANES, SUBLANES)
    moved = []
    for d in range(1, chips):
        peer = lax.rem(place + d, chips)
        moved.append(
            remote(
                g.mixed.at[:, pl.ds(peer * pieces, pieces)], g.joined.at[:, :, lines, :],
                g.s_mixed.at[d], g.r_mixed.at[d], peer // n_col * 2 + core, lax.rem(peer, n_col),
            )
        )
    start_all(moved)
    g.joined[:, :, lines, :] = g.mixed[:, pl.ds(place * pieces, pieces)]
    settle_turned(g.gram_sum.at[1], g.basis_two)
    basis_two = g.basis_two[...]
    f2_ref[...] = basis_two * math.sqrt(n_two)
    for copy in moved:
        copy.wait()
    for a in range(pieces):
        g.slab[a * rank : (a + 1) * rank, :] = product(
            basis_two, jnp.concatenate([g.joined[w, a] for w in range(portions)], axis=1)
        )

    chunk = rank // plane
    own_chunk = aligned(chip * chunk, chunk)

    def pair(source, target, send, recv):
        copy = remote(source, target, send, recv, other, col)
        copy.start()
        return copy

    def one(step, carry):
        iterate = product(linv_ref[...], g.image[step])
        g.cross_own[step] = right_product(iterate, g.slab[...])
        crossing = pair(g.cross_own.at[step], g.cross_pair.at[step], g.s_cross.at[step], g.r_cross.at[step])
        g.inner_own[step] = right_product(iterate, iterate)
        meeting = pair(g.inner_own.at[step], g.inner_pair.at[step], g.s_inner.at[step], g.r_inner.at[step])
        crossing.wait()
        g.image_part[step] = product(g.cross_own[step] + g.cross_pair[step], g.slab[...])
        first = start_all(
            [
                remote(
                    g.image_part.at[step, aligned(plane_peer(d) * chunk, chunk), :], g.image_parts.at[step, d],
                    g.s_image_row.at[step, d], g.r_image_row.at[step, d], plane_peer(d) * 2 + core, col,
                )
                for d in range(1, plane)
            ]
        )
        meeting.wait()
        total = g.image_part[step, own_chunk, :]
        for d in range(1, plane):
            first[d - 1].wait_recv()
            total = total + g.image_parts[step, d]
        g.image_planes[step, col] = total
        second = start_all(
            [
                remote(
                    g.image_planes.at[step, col], g.image_planes.at[step, col],
                    g.s_image_col.at[step, d], g.r_image_col.at[step, d], row, col_peer(d),
                )
                for d in range(1, n_col)
            ]
        )
        inverse = inverse_factor(g.inner_own[step] + g.inner_pair[step])
        linv_ref[...] = jnp.where(step == 0, unit(rank), inverse)
        for copy in second:
            copy.wait_recv()
        total = g.image_planes[step, 0]
        for q in range(1, n_col):
            total = total + g.image_planes[step, q]
        g.image[step + 1, own_chunk, :] = total
        third = start_all(
            [
                remote(
                    g.image.at[step + 1, own_chunk, :], g.image.at[step + 1, own_chunk, :],
                    g.s_image_all.at[step, d], g.r_image_all.at[step, d], plane_peer(d) * 2 + core, col,
                )
                for d in range(1, plane)
            ]
        )
        for copy in third:
            copy.wait_recv()
        for copy in first + second + third:
            copy.wait_send()
        return carry

    lax.fori_loop(0, STEPS, one, 0)
    iterate = product(linv_ref[...], g.image[STEPS])
    g.core_own[...] = right_product(g.slab[...], iterate)
    crossing = pair(g.core_own, g.core_pair, g.s_last.at[0], g.r_last.at[0])
    g.inner_own[STEPS] = right_product(iterate, iterate)
    meeting = pair(g.inner_own.at[STEPS], g.inner_pair.at[STEPS], g.s_inner.at[STEPS], g.r_inner.at[STEPS])
    mine = aligned(core * half, half, LANES)
    g.last[...] = iterate
    last_ref[:, mine] = iterate
    lasting = pair(g.last, last_ref.at[:, mine], g.s_last.at[1], g.r_last.at[1])
    crossing.wait()
    g.core_sum[...] = (g.core_own[...] + g.core_pair[...]).reshape(pieces, rank, rank)
    own_b = rank // n_col
    own_pieces = pl.ds(col * pieces, pieces)
    moved = start_all(
        [
            remote(
                g.core_sum.at[:, aligned(col_peer(d) * own_b, own_b), :], g.core_all.at[own_pieces],
                g.s_core.at[d], g.r_core.at[d], row, col_peer(d),
            )
            for d in range(1, n_col)
        ]
    )
    g.core_all[own_pieces] = g.core_sum[:, aligned(col * own_b, own_b), :]
    meeting.wait()
    linv_ref[...] = inverse_factor(g.inner_own[STEPS] + g.inner_pair[STEPS])
    lasting.wait()
    for copy in moved:
        copy.wait()
    own_a = piece_ref.shape[0]
    piece_ref[...] = g.core_all[pl.ds(core * own_a, own_a)]


def finish_kernel(one_ref, two_ref, last_ref, linv_ref, piece_ref, f1_ref, f2_ref, f3_ref, core_ref):
    f1_ref[...] = one_ref[...]
    f2_ref[...] = two_ref[...]
    linv = linv_ref[...]
    f3_ref[...] = product(linv, last_ref[...]) * math.sqrt(last_ref.shape[1])
    core_ref[...] = right_product(piece_ref[...].reshape(core_ref.shape), linv)


def unit(size):
    shape = (size, size)
    return (lax.broadcasted_iota(jnp.int32, shape, 0) == lax.broadcasted_iota(jnp.int32, shape, 1)).astype(jnp.float32)


def shared(n_row, n_col, tensor, start_one, start_two, start_three):
    rows_one, rows_two, depth = tensor.shape
    rank = start_three.shape[1]
    own_a, own_b = rank // n_row, rank // n_col
    spec = pl.BlockSpec(memory_space=pltpu.VMEM)
    scratch = chain_scratch(n_row, n_col, rows_one, rows_two, depth, rank)

    def outs(*shapes):
        return [jax.ShapeDtypeStruct(shape, jnp.float32) for shape in shapes]

    chained = pl.pallas_call(
        functools.partial(chain_kernel, n_row, n_col, tuple(scratch)),
        out_shape=outs((rank, LANES), (rank, LANES), (rank, depth), (rank, rank), (own_a, own_b, rank)),
        in_specs=[spec] * 4,
        out_specs=[spec] * 5,
        scratch_shapes=list(scratch.values()),
        compiler_params=pltpu.CompilerParams(
            collective_id=1, has_side_effects=True, vmem_limit_bytes=48 * 2**20
        ),
        cost_estimate=pl.CostEstimate(flops=10**9, bytes_accessed=10**7, transcendentals=0),
        name="chain",
    )(tensor, start_three.T, start_one, start_two)
    factor_one, factor_two, factor_three, core = pl.pallas_call(
        finish_kernel,
        out_shape=outs((rank, LANES), (rank, LANES), (rank, depth), (own_a * own_b, rank)),
        in_specs=[spec] * 5,
        out_specs=[spec] * 4,
        cost_estimate=pl.CostEstimate(flops=10**7, bytes_accessed=10**6, transcendentals=0),
        name="finish",
    )(*chained)
    return (factor_one.T, factor_two.T, factor_three.T, core.reshape(own_a, own_b, rank).transpose(2, 0, 1))


def solution(mesh):
    n_row, n_col = mesh.shape["row"], mesh.shape["col"]
    n = n_row * n_col

    def on_device(tensor, start_one, start_two, start_three):
        rows_one, rows_two, depth = tensor.shape
        rank = start_three.shape[1]
        plane, span = n_row // 2, rows_one * rows_two
        even = (
            n_row % 2 == 0
            and rows_one * n_row == rows_two * n_col == LANES
            and rows_two == plane * SUBLANES
            and rows_one % SUBLANES == 0
            and depth % (2 * LANES) == 0
            and rank % (plane * SUBLANES) == 0
            and rank % (n_col * SUBLANES) == 0
            and rank % n == 0
            and rank // n * (span // LANES) == SUBLANES
        )
        if even:
            return shared(n_row, n_col, tensor, start_one, start_two, start_three)
        return general(tensor, start_one, start_two, start_three)

    return jax.shard_map(
        on_device,
        mesh=mesh,
        in_specs=(P("row", "col", None), P("row", None), P("col", None), P()),
        out_specs=(P(), P(), P(), P(None, "row", "col")),
        check_vma=False,
    )
```

```python
import functools
import math
import types

import jax
import jax.numpy as jnp
from jax import lax
from jax.experimental import pallas as pl
from jax.experimental.pallas import tpu as pltpu
from jax.sharding import PartitionSpec as P

STEPS = 4


HIGHEST = lax.Precision.HIGHEST
MESH = pl.DeviceIdType.MESH
SUBLANES = 8
LANES = 128


def product(left, right):
    return jnp.dot(left, right, precision=HIGHEST, preferred_element_type=jnp.float32)


def left_product(left, right):
    return lax.dot_general(
        left, right, (((0,), (0,)), ((), ())), precision=HIGHEST, preferred_element_type=jnp.float32
    )


def right_product(left, right):
    return lax.dot_general(
        left, right, (((1,), (1,)), ((), ())), precision=HIGHEST, preferred_element_type=jnp.float32
    )


def cross_product(left, right):
    return lax.dot_general(
        left, right, (((0,), (1,)), ((), ())), precision=HIGHEST, preferred_element_type=jnp.float32
    )


def orthonormal(matrix, inner):
    lower = jnp.linalg.cholesky(inner)
    return jax.scipy.linalg.solve_triangular(lower, matrix.T, lower=True).T


def settle(gram_whole, basis):
    for iteration in range(STEPS):
        image = product(gram_whole, basis)
        basis = orthonormal(image, left_product(image, image))
    return basis


def general(tensor, start_one, start_two, start_three):
    rows_one, rows_two, depth = tensor.shape
    rank = start_three.shape[1]
    flat = tensor.reshape(rows_one * rows_two, depth)
    contracted = cross_product(start_three, flat).reshape(rank, rows_one, rows_two)
    part_one = jnp.einsum("cij,jb->ibc", contracted, start_two, precision=HIGHEST).reshape(
        rows_one, rank * rank
    )
    slab_one = lax.psum_scatter(part_one, "col", scatter_dimension=1, tiled=True)
    slab_rows_one = lax.all_gather(slab_one, "row", axis=0, tiled=True)
    gram_one = lax.psum(right_product(slab_rows_one, slab_rows_one), "col")
    basis_one = settle(gram_one, lax.all_gather(start_one, "row", axis=0, tiled=True))
    own_one = lax.dynamic_slice_in_dim(basis_one, lax.axis_index("row") * rows_one, rows_one, 0)
    part_two = jnp.einsum("cij,ia->jac", contracted, own_one, precision=HIGHEST).reshape(
        rows_two, rank * rank
    )
    slab_two = lax.psum_scatter(part_two, "row", scatter_dimension=1, tiled=True)
    slab_rows_two = lax.all_gather(slab_two, "col", axis=0, tiled=True)
    gram_two = lax.psum(right_product(slab_rows_two, slab_rows_two), "row")
    basis_two = settle(gram_two, lax.all_gather(start_two, "col", axis=0, tiled=True))
    own_two = lax.dynamic_slice_in_dim(basis_two, lax.axis_index("col") * rows_two, rows_two, 0)
    received = lax.all_to_all(tensor, "row", split_axis=2, concat_axis=0, tiled=True)
    count, items, cells = received.shape
    merged = left_product(basis_one, received.reshape(count, items * cells))
    mixed = merged.reshape(rank, items, cells)
    part_three = jnp.einsum("ajk,jb->kba", mixed, own_two, precision=HIGHEST)
    cells_here = part_three.shape[0]
    slab_three = lax.psum_scatter(
        part_three.reshape(cells_here, rank * rank), "col", scatter_dimension=1, tiled=True
    )
    gram_part_three = right_product(slab_three, lax.all_gather(slab_three, "row", axis=0, tiled=True))
    gram_three = lax.psum(gram_part_three, "col")
    basis_three = start_three
    own_three = start_three
    for iteration in range(STEPS):
        image = product(gram_three, basis_three)
        inner = lax.psum(left_product(image, image), "row")
        own_three = orthonormal(image, inner)
        basis_three = lax.all_gather(own_three, "row", axis=0, tiled=True)
    core_part = left_product(own_three, slab_three)
    core_part = core_part.reshape(rank, core_part.shape[1] // rank, rank)
    core = lax.psum_scatter(core_part, "row", scatter_dimension=2, tiled=True).transpose(0, 2, 1)
    factor_one = basis_one * math.sqrt(basis_one.shape[0])
    factor_two = basis_two * math.sqrt(basis_two.shape[0])
    factor_three = basis_three * math.sqrt(basis_three.shape[0])
    return (factor_one, factor_two, factor_three, core)


def inverse_factor(inner):
    n = inner.shape[0]
    groups = n // SUBLANES
    eye = (
        lax.broadcasted_iota(jnp.int32, (n, n), 0) == lax.broadcasted_iota(jnp.int32, (n, n), 1)
    ).astype(jnp.float32)
    whole = jnp.concatenate([inner, eye], axis=1)
    width = whole.shape[1]
    rows = [whole[g * SUBLANES : (g + 1) * SUBLANES] for g in range(groups)]
    sub = lax.broadcasted_iota(jnp.int32, (SUBLANES, width), 0)
    pivots = [None] * n
    shape = (SUBLANES, width)
    for base in range(groups):
        columns = [
            [jnp.broadcast_to(rows[g][:, k : k + 1], shape) for g in range(base, groups)]
            for k in range(base * SUBLANES, (base + 1) * SUBLANES)
        ]
        for t in range(SUBLANES):
            pivot = jnp.broadcast_to(columns[t][0][t : t + 1, :], shape)
            scale = 1.0 / pivot
            pivots[base * SUBLANES + t] = pivot
            row = jnp.broadcast_to(rows[base][t : t + 1, :], shape)
            heads = [
                jnp.broadcast_to(columns[s][0][t : t + 1, :], shape) for s in range(t + 1, SUBLANES)
            ]
            for g in range(base, groups):
                factor = columns[t][g - base] * scale
                if g == base:
                    factor = jnp.where(sub > t, factor, 0.0)
                rows[g] = rows[g] - factor * row
                for s in range(t + 1, SUBLANES):
                    columns[s][g - base] = columns[s][g - base] - factor * heads[s - t - 1]
    out = []
    for g in range(groups):
        held = pivots[g * SUBLANES]
        for t in range(1, SUBLANES):
            held = jnp.where(sub == t, pivots[g * SUBLANES + t], held)
        out.append(rows[g] * lax.rsqrt(held))
    return jnp.concatenate(out, axis=0)[:, n:]


def lane_groups(width):
    return lax.div(lax.broadcasted_iota(jnp.int32, (1, LANES), 1), width)


def shifted(value, amount):
    amount = amount % LANES
    return value if amount == 0 else pltpu.roll(value, amount, 1)


def settle_turned(gram_ref, basis_ref):
    basis_ref[...] = product(basis_ref[...], gram_ref[...])

    def one(_, carry):
        image = basis_ref[...]
        further = product(image, gram_ref[...])
        basis_ref[...] = product(inverse_factor(right_product(image, image)), further)
        return carry

    lax.fori_loop(0, STEPS - 1, one, 0)
    image = basis_ref[...]
    basis_ref[...] = product(inverse_factor(right_product(image, image)), image)


def aligned(start, count, multiple=SUBLANES):
    return pl.ds(pl.multiple_of(start, multiple), count)


def remote(source, target, sems, row, col):
    return pltpu.make_async_remote_copy(
        src_ref=source, dst_ref=target, send_sem=sems[0], recv_sem=sems[1], device_id=(row, col), device_id_type=MESH
    )


def start_all(made):
    for copy in made:
        copy.start()


def wait_bytes(ref, sem):
    pltpu.make_async_copy(ref, ref, sem).wait()


def chain_scratch(n_row, n_col, rows_one, rows_two, depth, rank):
    n, chips, plane = n_row * n_col, n_row * n_col // 2, n_row // 2
    half, blocks, chunk, n_one, n_two = depth // 2, rank // chips, rank // plane, LANES, LANES
    share, portions, own_b = rank // n, half // LANES, rank // n_col

    def buffer(*shape):
        return pltpu.VMEM(shape, jnp.float32)

    def dma(*shape):
        return pltpu.SemaphoreType.DMA(shape)

    return dict(
        tensor=buffer(rows_one, rows_two, depth),
        start=buffer(rank, depth),
        part_one=buffer(rows_one, rank),
        part_two=buffer(rows_two, rank),
        parted=buffer(n * SUBLANES, LANES),
        held=buffer(n * SUBLANES, LANES),
        faces=buffer(share * n_one, n_two),
        turned=buffer(share, n_two, n_one),
        all_one=buffer(n_one, rank),
        all_two=buffer(n_two, rank),
        gram_part=buffer(2, LANES, LANES),
        gram_parts=buffer(2, n_row, LANES // n_row, LANES),
        gram_planes=buffer(2, n_col, LANES // n_row, LANES),
        gram_sum=buffer(2, LANES, LANES),
        basis_one=buffer(rank, n_one),
        basis_two=buffer(rank, n_two),
        factors=buffer(2, rank, LANES),
        block=buffer(portions, n_one, SUBLANES, LANES),
        mixed=buffer(portions, rank, SUBLANES, LANES),
        joined=buffer(portions, blocks, n_two, LANES),
        slab=buffer(blocks * rank, half),
        linv=buffer(rank, rank),
        image=buffer(STEPS + 1, portions, rank, LANES),
        cross_own=buffer(STEPS, rank, blocks * rank),
        cross_pair=buffer(STEPS, rank, blocks * rank),
        inner_own=buffer(STEPS + 1, rank, rank),
        inner_pair=buffer(STEPS + 1, rank, rank),
        image_part=buffer(STEPS, portions, rank, LANES),
        image_parts=buffer(STEPS, portions, plane, chunk, LANES),
        image_planes=buffer(STEPS, portions, n_col, chunk, LANES),
        last=buffer(2, rank, half),
        core_own=buffer(blocks * rank, rank),
        core_pair=buffer(blocks * rank, rank),
        core_sum=buffer(blocks, rank, rank),
        core_all=buffer(n_col * blocks, own_b, rank),
        loaded=dma(4),
        stored=dma(6),
        d_held=dma(2),
        d_one=dma(2),
        d_two=dma(2),
        d_block=dma(2),
        kept=dma(1),
        d_gram_row=dma(2, 2),
        d_gram_col=dma(2, 2),
        d_gram_all=dma(2, 2),
        d_mixed=dma(2),
        d_cross=dma(2, 2),
        d_inner=dma(2, 2),
        d_image_row=dma(portions, 2),
        d_image_col=dma(2, portions, 2),
        d_image_all=dma(portions, 2),
        d_last=dma(2),
        d_wide=dma(2),
        d_core=dma(2),
    )


def chain_kernel(n_row, n_col, names, *refs):
    ins, outs, refs = refs[:4], refs[4:9], refs[9:]
    g = types.SimpleNamespace(**dict(zip(names, refs)))
    t_ref, v_ref = g.tensor, g.start
    row, col = lax.axis_index("row"), lax.axis_index("col")
    n, plane, chips = n_row * n_col, n_row // 2, n_row * n_col // 2
    me, chip, core = row * n_col + col, row // 2, lax.rem(row, 2)
    other = row + 1 - 2 * core
    rows_one, rows_two, depth = t_ref.shape
    rank, half = v_ref.shape[0], depth // 2
    share, tiles, portions = rank // n, rows_one * rows_two // LANES, half // LANES
    n_one = n_two = LANES
    row_peers = [lax.rem(row + d, n_row) for d in range(n_row)]
    col_peers = [lax.rem(col + d, n_col) for d in range(n_col)]
    chip_peers = [lax.rem(chip + d, plane) for d in range(plane)]
    far = sorted(
        [(a, b) for a in range(n_row) for b in range(n_col) if a or b], key=lambda at: -min(at[1], n_col - at[1])
    )

    def pair(sems, k):
        return (sems.at[k, 0], sems.at[k, 1])

    def ends(sems):
        return (sems.at[0], sems.at[1])

    parts = (t_ref, v_ref, g.part_one, g.part_two)
    loads = [pltpu.make_async_copy(ins[k], parts[k], g.loaded.at[k]) for k in range(4)]
    start_all(loads)
    barrier = pltpu.get_barrier_semaphore()
    for a, b in far:
        pl.semaphore_signal(barrier, inc=1, device_id=(row_peers[a], col_peers[b]), device_id_type=MESH)
    for copy in loads:
        copy.wait()
    contracted = right_product(v_ref[...], t_ref[...].reshape(rows_one * rows_two, depth))
    for tile in range(tiles):
        g.parted[pl.ds(tile, rank, stride=tiles), :] = contracted[:, tile * LANES : (tile + 1) * LANES]
    pl.semaphore_wait(barrier, n - 1)
    place = aligned((col * n_row + row) * SUBLANES, SUBLANES)
    start_all(
        [
            remote(
                g.parted.at[aligned((row_peers[a] * n_col + col_peers[b]) * SUBLANES, SUBLANES), :],
                g.held.at[place, :], ends(g.d_held), row_peers[a], col_peers[b],
            )
            for a, b in far
        ]
    )
    own_one, own_two = aligned(row * rows_one, rows_one), aligned(col * rows_two, rows_two)
    start_all([remote(g.part_two, g.all_two.at[own_two, :], ends(g.d_two), row, col_peers[d]) for d in range(1, n_col)])
    start_all([remote(g.part_one, g.all_one.at[own_one, :], ends(g.d_one), row_peers[d], col) for d in range(1, n_row)])

    def block_source(which, peer):
        return t_ref.at[
            :,
            aligned(peer // 2 * SUBLANES, SUBLANES),
            aligned(lax.rem(peer, 2) * half + which * LANES, LANES, LANES),
        ]

    def block_target(which):
        return g.block.at[which, pl.ds(row * rows_one, rows_one)]

    def block_start(which):
        start_all(
            [
                remote(block_source(which, row_peers[d]), block_target(which), ends(g.d_block), row_peers[d], col)
                for d in range(1, n_row)
            ]
        )

    block_start(0)
    start_all([pltpu.make_async_copy(block_source(w, row), block_target(w), g.kept.at[0]) for w in range(portions)])
    g.held[place, :] = g.parted[aligned(me * SUBLANES, SUBLANES), :]
    g.all_one[own_one, :] = g.part_one[...]
    g.all_two[own_two, :] = g.part_two[...]
    for w in range(portions):
        g.image[0, w] = v_ref[:, aligned(core * half + w * LANES, LANES, LANES)]
    g.linv[...] = unit(rank)
    for end in range(2):
        wait_bytes(g.all_two.at[pl.ds(0, n_two - rows_two), :], g.d_two.at[end])
        wait_bytes(g.all_one.at[pl.ds(0, n_one - rows_one), :], g.d_one.at[end])
        wait_bytes(g.held.at[pl.ds(0, (n - 1) * SUBLANES), :], g.d_held.at[end])
    group = lane_groups(rows_two)
    for c in range(share):
        for tile in range(tiles):
            blocks = [
                g.held[pl.ds(q * n_row * SUBLANES + c * tiles + tile, n_row, stride=SUBLANES), :] for q in range(n_col)
            ]
            for s in range(n_col):
                line = shifted(blocks[0], -s * rows_two)
                for q in range(1, n_col):
                    line = jnp.where(group == q, shifted(blocks[q], (q - s) * rows_two), line)
                g.faces[pl.ds(c * n_one + tile * n_col + s, n_row, stride=rows_one), :] = line

    count = LANES // n_row
    own_rows = aligned(row * count, count)

    def gram_first(w):
        start_all(
            [
                remote(
                    g.gram_part.at[w, aligned(row_peers[d] * count, count), :], g.gram_parts.at[w, d],
                    pair(g.d_gram_row, w), row_peers[d], col,
                )
                for d in range(1, n_row)
            ]
        )

    def gram_second(w):
        wait_bytes(g.gram_parts.at[w, pl.ds(0, n_row - 1)], g.d_gram_row.at[w, 1])
        total = g.gram_part[w, own_rows, :]
        for d in range(1, n_row):
            total = total + g.gram_parts[w, d]
        g.gram_planes[w, col] = total
        start_all(
            [
                remote(g.gram_planes.at[w, col], g.gram_planes.at[w, col], pair(g.d_gram_col, w), row, col_peers[d])
                for d in range(1, n_col)
            ]
        )

    def gram_third(w):
        wait_bytes(g.gram_planes.at[w, pl.ds(0, n_col - 1)], g.d_gram_col.at[w, 1])
        total = g.gram_planes[w, 0]
        for q in range(1, n_col):
            total = total + g.gram_planes[w, q]
        g.gram_sum[w, own_rows, :] = total
        start_all(
            [
                remote(
                    g.gram_sum.at[w, own_rows, :], g.gram_sum.at[w, own_rows, :],
                    pair(g.d_gram_all, w), row_peers[d], col,
                )
                for d in range(1, n_row)
            ]
        )

    def gram_end(w):
        wait_bytes(g.gram_sum.at[w, pl.ds(0, LANES - count), :], g.d_gram_all.at[w, 1])
        wait_bytes(g.gram_parts.at[w, pl.ds(0, n_row - 1)], g.d_gram_row.at[w, 0])
        wait_bytes(g.gram_planes.at[w, pl.ds(0, n_col - 1)], g.d_gram_col.at[w, 0])
        wait_bytes(g.gram_sum.at[w, pl.ds(0, LANES - count), :], g.d_gram_all.at[w, 0])

    def self_gram(slabs):
        total = right_product(slabs[0], slabs[0])
        for slab in slabs[1:]:
            total = total + right_product(slab, slab)
        return total

    g.gram_part[0] = self_gram(
        [product(g.faces[c * n_one : (c + 1) * n_one, :], g.all_two[...]) for c in range(share)]
    )
    gram_first(0)
    for c in range(share):
        g.turned[c] = g.faces[c * n_one : (c + 1) * n_one, :].T
    g.basis_one[...] = g.all_one[...].T
    g.basis_two[...] = g.all_two[...].T
    gram_second(0)
    block_start(1)
    gram_third(0)
    gram_end(0)
    for which in range(2, portions):
        block_start(which)
    settle_turned(g.gram_sum.at[0], g.basis_one)
    basis_one = g.basis_one[...]

    g.gram_part[1] = self_gram([right_product(g.turned[c], basis_one) for c in range(share)])
    gram_first(1)
    g.factors[0] = basis_one * math.sqrt(n_one)
    for end in range(2):
        wait_bytes(g.block.at[:, pl.ds(0, n_one - rows_one)], g.d_block.at[end])
    wait_bytes(g.block.at[:, pl.ds(0, rows_one)], g.kept.at[0])
    flat_block = g.block.reshape(portions * n_one * SUBLANES, LANES)
    flat_mixed = g.mixed.reshape(portions * rank * SUBLANES, LANES)
    for s in range(SUBLANES):
        face = [flat_block[pl.ds(w * n_one * SUBLANES + s, n_one, stride=SUBLANES), :] for w in range(portions)]
        face = product(basis_one, jnp.concatenate(face, axis=1))
        for w in range(portions):
            flat_mixed[pl.ds(w * rank * SUBLANES + s, rank, stride=SUBLANES), :] = face[:, w * LANES : (w + 1) * LANES]
    gram_second(1)
    pieces = rank // chips
    place = chip * n_col + col
    lines = aligned(col * rows_two + chip * SUBLANES, SUBLANES)
    start_all(
        [
            remote(
                g.mixed.at[:, pl.ds((chip_peers[a] * n_col + col_peers[b]) * pieces, pieces)], g.joined.at[:, :, lines, :],
                ends(g.d_mixed), chip_peers[a] * 2 + core, col_peers[b],
            )
            for a, b in far
            if a < plane
        ]
    )
    gram_third(1)
    g.joined[:, :, lines, :] = g.mixed[:, pl.ds(place * pieces, pieces)]
    gram_end(1)
    settle_turned(g.gram_sum.at[1], g.basis_two)
    basis_two = g.basis_two[...]
    g.factors[1] = basis_two * math.sqrt(n_two)
    stores = [pltpu.make_async_copy(g.factors.at[k], outs[k], g.stored.at[k]) for k in range(2)]
    start_all(stores)
    for end in range(2):
        wait_bytes(g.mixed.at[:, pl.ds(0, rank - pieces)], g.d_mixed.at[end])
    for a in range(pieces):
        g.slab[a * rank : (a + 1) * rank, :] = product(
            basis_two, jnp.concatenate([g.joined[w, a] for w in range(portions)], axis=1)
        )

    chunk = rank // plane
    own_chunk = aligned(chip * chunk, chunk)

    def swap(source, target, sems):
        copy = remote(source, target, ends(sems), other, col)
        copy.start()
        return copy

    def lanes(value, w):
        return value[:, w * LANES : (w + 1) * LANES]

    def scaled(step, w):
        return product(g.linv[...], g.image[step, w])

    def one(step, carry):
        turn = lax.rem(step, 2)
        iterate, cross, inner = [], None, None
        for w in range(portions):
            @pl.when(step > 0)
            def _():
                wait_bytes(g.image.at[step, w, pl.ds(0, rank - chunk), :], g.d_image_all.at[w, 1])
                wait_bytes(g.image.at[step, w, pl.ds(0, rank - chunk), :], g.d_image_all.at[w, 0])

            now = scaled(step, w)
            iterate.append(now)
            term = right_product(now, g.slab[:, w * LANES : (w + 1) * LANES])
            cross = term if cross is None else cross + term
        g.cross_own[step] = cross
        crossing = swap(g.cross_own.at[step], g.cross_pair.at[step], g.d_cross.at[turn])
        for now in iterate:
            term = right_product(now, now)
            inner = term if inner is None else inner + term
        g.inner_own[step] = inner
        meeting = swap(g.inner_own.at[step], g.inner_pair.at[step], g.d_inner.at[turn])
        crossing.wait()
        cross = g.cross_own[step] + g.cross_pair[step]
        for w in range(portions):
            g.image_part[step, w] = product(cross, g.slab[:, w * LANES : (w + 1) * LANES])
            start_all(
                [
                    remote(
                        g.image_part.at[step, w, aligned(chip_peers[d] * chunk, chunk), :], g.image_parts.at[step, w, d],
                        pair(g.d_image_row, w), chip_peers[d] * 2 + core, col,
                    )
                    for d in range(1, plane)
                ]
            )
        meeting.wait()
        for w in range(portions):
            wait_bytes(g.image_parts.at[step, w, pl.ds(0, plane - 1)], g.d_image_row.at[w, 1])
            total = g.image_part[step, w, own_chunk, :]
            for d in range(1, plane):
                total = total + g.image_parts[step, w, d]
            g.image_planes[step, w, col] = total
            start_all(
                [
                    remote(
                        g.image_planes.at[step, w, col], g.image_planes.at[step, w, col],
                        pair(g.d_image_col.at[turn], w), row, col_peers[d],
                    )
                    for d in range(1, n_col)
                ]
            )
        inverse = inverse_factor(g.inner_own[step] + g.inner_pair[step])
        g.linv[...] = jnp.where(step == 0, unit(rank), inverse)
        for w in range(portions):
            wait_bytes(g.image_planes.at[step, w, pl.ds(0, n_col - 1)], g.d_image_col.at[turn, w, 1])
            total = g.image_planes[step, w, 0]
            for q in range(1, n_col):
                total = total + g.image_planes[step, w, q]
            g.image[step + 1, w, own_chunk, :] = total
            start_all(
                [
                    remote(
                        g.image.at[step + 1, w, own_chunk, :], g.image.at[step + 1, w, own_chunk, :],
                        pair(g.d_image_all, w), chip_peers[d] * 2 + core, col,
                    )
                    for d in range(1, plane)
                ]
            )
        for w in range(portions):
            wait_bytes(g.image_parts.at[step, w, pl.ds(0, plane - 1)], g.d_image_row.at[w, 0])
            wait_bytes(g.image_planes.at[step, w, pl.ds(0, n_col - 1)], g.d_image_col.at[turn, w, 0])
        return carry

    lax.fori_loop(0, STEPS, one, 0)
    inner, cross = None, None
    for w in range(portions):
        for end in (1, 0):
            wait_bytes(g.image.at[STEPS, w, pl.ds(0, rank - chunk), :], g.d_image_all.at[w, end])
        now = scaled(STEPS, w)
        g.last[0, :, w * LANES : (w + 1) * LANES] = now
        term = right_product(g.slab[:, w * LANES : (w + 1) * LANES], now)
        cross = term if cross is None else cross + term
    g.core_own[...] = cross
    crossing = swap(g.core_own, g.core_pair, g.d_last)
    for w in range(portions):
        now = g.last[0, :, w * LANES : (w + 1) * LANES]
        term = right_product(now, now)
        inner = term if inner is None else inner + term
    g.inner_own[STEPS] = inner
    meeting = swap(g.inner_own.at[STEPS], g.inner_pair.at[STEPS], g.d_inner.at[STEPS % 2])
    lasting = swap(g.last.at[0], g.last.at[1], g.d_wide)
    crossing.wait()
    g.core_sum[...] = (g.core_own[...] + g.core_pair[...]).reshape(pieces, rank, rank)
    own_b = rank // n_col
    own_pieces = pl.ds(col * pieces, pieces)
    start_all(
        [
            remote(
                g.core_sum.at[:, aligned(col_peers[d] * own_b, own_b), :], g.core_all.at[own_pieces],
                ends(g.d_core), row, col_peers[d],
            )
            for d in range(1, n_col)
        ]
    )
    g.core_all[own_pieces] = g.core_sum[:, aligned(col * own_b, own_b), :]
    meeting.wait()
    lasting.wait()
    for k, owner in enumerate((core, 1 - core)):
        stores.append(
            pltpu.make_async_copy(
                g.last.at[k], outs[2].at[:, aligned(owner * half, half, LANES)], g.stored.at[2 + k]
            )
        )
        stores[-1].start()
    g.linv[...] = inverse_factor(g.inner_own[STEPS] + g.inner_pair[STEPS])
    stores.append(pltpu.make_async_copy(g.linv, outs[3], g.stored.at[4]))
    stores[-1].start()
    for end in (1, 0):
        wait_bytes(g.core_all.at[pl.ds(0, (n_col - 1) * pieces)], g.d_core.at[end])
    own_a = outs[4].shape[0]
    stores.append(pltpu.make_async_copy(g.core_all.at[pl.ds(core * own_a, own_a)], outs[4], g.stored.at[5]))
    stores[-1].start()
    for copy in stores:
        copy.wait()


def finish_kernel(one_ref, two_ref, last_ref, linv_ref, piece_ref, f1_ref, f2_ref, f3_ref, core_ref):
    f1_ref[...] = one_ref[...]
    f2_ref[...] = two_ref[...]
    linv = linv_ref[...]
    f3_ref[...] = product(linv, last_ref[...]) * math.sqrt(last_ref.shape[1])
    core_ref[...] = right_product(piece_ref[...].reshape(core_ref.shape), linv)


def unit(size):
    shape = (size, size)
    return (lax.broadcasted_iota(jnp.int32, shape, 0) == lax.broadcasted_iota(jnp.int32, shape, 1)).astype(jnp.float32)


def shared(n_row, n_col, tensor, start_one, start_two, start_three):
    rows_one, rows_two, depth = tensor.shape
    rank = start_three.shape[1]
    own_a, own_b = rank // n_row, rank // n_col
    spec = pl.BlockSpec(memory_space=pltpu.VMEM)
    scratch = chain_scratch(n_row, n_col, rows_one, rows_two, depth, rank)

    def outs(*shapes):
        return [jax.ShapeDtypeStruct(shape, jnp.float32) for shape in shapes]

    chained = pl.pallas_call(
        functools.partial(chain_kernel, n_row, n_col, tuple(scratch)),
        out_shape=outs((rank, LANES), (rank, LANES), (rank, depth), (rank, rank), (own_a, own_b, rank)),
        in_specs=[pl.BlockSpec(memory_space=pltpu.HBM)] * 4,
        out_specs=[pl.BlockSpec(memory_space=pltpu.HBM)] * 5,
        scratch_shapes=list(scratch.values()),
        compiler_params=pltpu.CompilerParams(
            collective_id=1, has_side_effects=True, vmem_limit_bytes=67043328 - 300 * 1024
        ),
        cost_estimate=pl.CostEstimate(flops=10**9, bytes_accessed=10**7, transcendentals=0),
        name="chain",
    )(tensor, start_three.T, start_one, start_two)
    factor_one, factor_two, factor_three, core = pl.pallas_call(
        finish_kernel,
        out_shape=outs((rank, LANES), (rank, LANES), (rank, depth), (own_a * own_b, rank)),
        in_specs=[spec] * 5,
        out_specs=[spec] * 4,
        compiler_params=pltpu.CompilerParams(vmem_limit_bytes=67043328 - 100 * 1024),
        cost_estimate=pl.CostEstimate(flops=10**7, bytes_accessed=10**6, transcendentals=0),
        name="finish",
    )(*chained)
    return (factor_one.T, factor_two.T, factor_three.T, core.reshape(own_a, own_b, rank).transpose(2, 0, 1))


def solution(mesh):
    n_row, n_col = mesh.shape["row"], mesh.shape["col"]
    n = n_row * n_col

    def on_device(tensor, start_one, start_two, start_three):
        rows_one, rows_two, depth = tensor.shape
        rank = start_three.shape[1]
        plane, span = n_row // 2, rows_one * rows_two
        even = (
            n_row % 2 == 0
            and rows_one * n_row == rows_two * n_col == LANES
            and rows_two == plane * SUBLANES
            and rows_one % SUBLANES == 0
            and depth % (2 * LANES) == 0
            and rank % (plane * SUBLANES) == 0
            and rank % (n_col * SUBLANES) == 0
            and rank % n == 0
            and rank // n * (span // LANES) == SUBLANES
        )
        if even:
            return shared(n_row, n_col, tensor, start_one, start_two, start_three)
        return general(tensor, start_one, start_two, start_three)

    return jax.shard_map(
        on_device,
        mesh=mesh,
        in_specs=(P("row", "col", None), P("row", None), P("col", None), P()),
        out_specs=(P(), P(), P(), P(None, "row", "col")),
        check_vma=False,
    )
```

```python
import functools
import math
import types

import jax
import jax.numpy as jnp
from jax import lax
from jax.experimental import pallas as pl
from jax.experimental.pallas import tpu as pltpu
from jax.sharding import PartitionSpec as P

STEPS = 4


HIGHEST = lax.Precision.HIGHEST
MESH = pl.DeviceIdType.MESH
SUBLANES = 8
LANES = 128
BAND = 2 * LANES


def product(left, right):
    return jnp.dot(left, right, precision=HIGHEST, preferred_element_type=jnp.float32)


def left_product(left, right):
    return lax.dot_general(
        left, right, (((0,), (0,)), ((), ())), precision=HIGHEST, preferred_element_type=jnp.float32
    )


def right_product(left, right):
    return lax.dot_general(
        left, right, (((1,), (1,)), ((), ())), precision=HIGHEST, preferred_element_type=jnp.float32
    )


def cross_product(left, right):
    return lax.dot_general(
        left, right, (((0,), (1,)), ((), ())), precision=HIGHEST, preferred_element_type=jnp.float32
    )


def orthonormal(matrix, inner):
    lower = jnp.linalg.cholesky(inner)
    return jax.scipy.linalg.solve_triangular(lower, matrix.T, lower=True).T


def settle(gram_whole, basis):
    for iteration in range(STEPS):
        image = product(gram_whole, basis)
        basis = orthonormal(image, left_product(image, image))
    return basis


def general(tensor, start_one, start_two, start_three):
    rows_one, rows_two, depth = tensor.shape
    rank = start_three.shape[1]
    flat = tensor.reshape(rows_one * rows_two, depth)
    contracted = cross_product(start_three, flat).reshape(rank, rows_one, rows_two)
    part_one = jnp.einsum("cij,jb->ibc", contracted, start_two, precision=HIGHEST).reshape(
        rows_one, rank * rank
    )
    slab_one = lax.psum_scatter(part_one, "col", scatter_dimension=1, tiled=True)
    slab_rows_one = lax.all_gather(slab_one, "row", axis=0, tiled=True)
    gram_one = lax.psum(right_product(slab_rows_one, slab_rows_one), "col")
    basis_one = settle(gram_one, lax.all_gather(start_one, "row", axis=0, tiled=True))
    own_one = lax.dynamic_slice_in_dim(basis_one, lax.axis_index("row") * rows_one, rows_one, 0)
    part_two = jnp.einsum("cij,ia->jac", contracted, own_one, precision=HIGHEST).reshape(
        rows_two, rank * rank
    )
    slab_two = lax.psum_scatter(part_two, "row", scatter_dimension=1, tiled=True)
    slab_rows_two = lax.all_gather(slab_two, "col", axis=0, tiled=True)
    gram_two = lax.psum(right_product(slab_rows_two, slab_rows_two), "row")
    basis_two = settle(gram_two, lax.all_gather(start_two, "col", axis=0, tiled=True))
    own_two = lax.dynamic_slice_in_dim(basis_two, lax.axis_index("col") * rows_two, rows_two, 0)
    received = lax.all_to_all(tensor, "row", split_axis=2, concat_axis=0, tiled=True)
    count, items, cells = received.shape
    merged = left_product(basis_one, received.reshape(count, items * cells))
    mixed = merged.reshape(rank, items, cells)
    part_three = jnp.einsum("ajk,jb->kba", mixed, own_two, precision=HIGHEST)
    cells_here = part_three.shape[0]
    slab_three = lax.psum_scatter(
        part_three.reshape(cells_here, rank * rank), "col", scatter_dimension=1, tiled=True
    )
    gram_part_three = right_product(slab_three, lax.all_gather(slab_three, "row", axis=0, tiled=True))
    gram_three = lax.psum(gram_part_three, "col")
    basis_three = start_three
    own_three = start_three
    for iteration in range(STEPS):
        image = product(gram_three, basis_three)
        inner = lax.psum(left_product(image, image), "row")
        own_three = orthonormal(image, inner)
        basis_three = lax.all_gather(own_three, "row", axis=0, tiled=True)
    core_part = left_product(own_three, slab_three)
    core_part = core_part.reshape(rank, core_part.shape[1] // rank, rank)
    core = lax.psum_scatter(core_part, "row", scatter_dimension=2, tiled=True).transpose(0, 2, 1)
    factor_one = basis_one * math.sqrt(basis_one.shape[0])
    factor_two = basis_two * math.sqrt(basis_two.shape[0])
    factor_three = basis_three * math.sqrt(basis_three.shape[0])
    return (factor_one, factor_two, factor_three, core)


def unit(size):
    shape = (size, size)
    return (lax.broadcasted_iota(jnp.int32, shape, 0) == lax.broadcasted_iota(jnp.int32, shape, 1)).astype(jnp.float32)


def inverse_factor(inner):
    n = inner.shape[0]
    groups = n // SUBLANES
    whole = jnp.concatenate([inner, unit(n)], axis=1)
    shape = (SUBLANES, whole.shape[1])
    rows = [whole[g * SUBLANES : (g + 1) * SUBLANES] for g in range(groups)]
    sub = lax.broadcasted_iota(jnp.int32, shape, 0)
    zero = rows[0] * 0.0

    def across(value, t):
        return jnp.broadcast_to(value[t : t + 1, :], shape)

    def column(g, k):
        return jnp.broadcast_to(rows[g][:, k : k + 1], shape)

    diagonal = [column(0, k) + zero for k in range(SUBLANES)]
    out = []
    for base in range(groups):
        head = base * SUBLANES
        panel = [[column(g, head + k) for g in range(base + 1, groups)] for k in range(SUBLANES)]
        coming = []
        if base + 1 < groups:
            coming = [column(base + 1, head + SUBLANES + k) for k in range(SUBLANES)]
            panel[0][0] = panel[0][0] + zero
        held = None
        for t in range(SUBLANES):
            pivot = across(diagonal[t], t)
            held = pivot if held is None else jnp.where(sub >= t, pivot, held)
            scale = 1.0 / pivot
            row = across(rows[base], t)
            heads = [across(diagonal[s], t) for s in range(t + 1, SUBLANES)]
            factor = jnp.where(sub > t, diagonal[t] * scale, 0.0)
            for s in range(t + 1, SUBLANES):
                diagonal[s] = diagonal[s] - factor * heads[s - t - 1]
            rows[base] = rows[base] - factor * row
            for k, g in enumerate(range(base + 1, groups)):
                factor = panel[t][k] * scale
                if k == 0:
                    coming = [coming[s] - factor * across(panel[t][0], s) for s in range(SUBLANES)]
                rows[g] = rows[g] - factor * row
                for s in range(t + 1, SUBLANES):
                    panel[s][k] = panel[s][k] - factor * heads[s - t - 1]
        out.append(rows[base] * lax.rsqrt(held))
        diagonal = coming
    return jnp.concatenate(out, axis=0)[:, n:]


def lane_groups(width):
    return lax.div(lax.broadcasted_iota(jnp.int32, (1, LANES), 1), width)


def shifted(value, amount):
    amount = amount % LANES
    return value if amount == 0 else pltpu.roll(value, amount, 1)


def settle_turned(gram_ref, basis_ref):
    basis_ref[...] = product(basis_ref[...], gram_ref[...])

    def one(_, carry):
        image = basis_ref[...]
        further = product(image, gram_ref[...])
        basis_ref[...] = product(inverse_factor(right_product(image, image)), further)
        return carry

    lax.fori_loop(0, STEPS - 1, one, 0)
    image = basis_ref[...]
    basis_ref[...] = product(inverse_factor(right_product(image, image)), image)


def aligned(start, count, multiple=SUBLANES):
    return pl.ds(pl.multiple_of(start, multiple), count)


def remote(source, target, sems, row, col):
    return pltpu.make_async_remote_copy(
        src_ref=source, dst_ref=target, send_sem=sems[0], recv_sem=sems[1], device_id=(row, col), device_id_type=MESH
    )


def start_all(made):
    for copy in made:
        copy.start()


def wait_bytes(ref, sem):
    pltpu.make_async_copy(ref, ref, sem).wait()


def chain_scratch(n_row, n_col, rows_one, rows_two, depth, rank):
    n, half, n_one, n_two = n_row * n_col, depth // 2, LANES, LANES
    share, portions, pieces = rank // n, half // LANES, rank // n
    bands, chunk, own_b = depth // BAND, rank // n_row, rank // n_col

    def buffer(*shape):
        return pltpu.VMEM(shape, jnp.float32)

    def dma(*shape):
        return pltpu.SemaphoreType.DMA(shape)

    return dict(
        tensor=buffer(rows_one, rows_two, depth),
        start=buffer(rank, depth),
        part_one=buffer(rows_one, rank),
        part_two=buffer(rows_two, rank),
        parted=buffer(n * SUBLANES, LANES),
        held=buffer(n * SUBLANES, LANES),
        faces=buffer(share * n_one, n_two),
        turned=buffer(share, n_two, n_one),
        all_one=buffer(n_one, rank),
        all_two=buffer(n_two, rank),
        gram_part=buffer(2, LANES, LANES),
        gram_parts=buffer(2, n_row, LANES // n_row, LANES),
        gram_planes=buffer(2, n_col, LANES // n_row, LANES),
        gram_sum=buffer(2, LANES, LANES),
        basis_one=buffer(rank, n_one),
        basis_two=buffer(rank, n_two),
        factors=buffer(2, rank, LANES),
        block=buffer(portions, n_one, SUBLANES, LANES),
        mixed=buffer(portions, rank, SUBLANES, LANES),
        joined=buffer(2 * portions, pieces, n_two, LANES),
        slab=buffer(pieces * rank, depth),
        linv=buffer(rank, rank),
        iterate=buffer(rank, depth),
        cross=buffer(rank, pieces * rank),
        image=buffer(STEPS, bands, rank, BAND),
        image_part=buffer(STEPS, bands, rank, BAND),
        image_parts=buffer(STEPS, bands, n_row, chunk, BAND),
        image_planes=buffer(STEPS, bands, n_col, chunk, BAND),
        core_own=buffer(pieces, rank, rank),
        core_all=buffer(n_col * pieces, own_b, rank),
        loaded=dma(4),
        stored=dma(5),
        d_held=dma(2),
        d_one=dma(2),
        d_two=dma(2),
        d_block=dma(2),
        kept=dma(1),
        d_gram_row=dma(2, 2),
        d_gram_col=dma(2, 2),
        d_gram_all=dma(2, 2),
        d_mixed=dma(2),
        d_image_row=dma(bands, 2),
        d_image_col=dma(2, bands, 2),
        d_image_all=dma(bands, 2),
        d_core=dma(2),
    )


def chain_kernel(n_row, n_col, names, *refs):
    ins, outs, refs = refs[:4], refs[4:9], refs[9:]
    g = types.SimpleNamespace(**dict(zip(names, refs)))
    t_ref, v_ref = g.tensor, g.start
    row, col = lax.axis_index("row"), lax.axis_index("col")
    n = n_row * n_col
    me, chip, core = row * n_col + col, row // 2, lax.rem(row, 2)
    rows_one, rows_two, depth = t_ref.shape
    rank, half = v_ref.shape[0], depth // 2
    share, tiles, portions = rank // n, rows_one * rows_two // LANES, half // LANES
    n_one = n_two = LANES
    row_peers = [lax.rem(row + d, n_row) for d in range(n_row)]
    col_peers = [lax.rem(col + d, n_col) for d in range(n_col)]
    far = sorted(
        [(a, b) for a in range(n_row) for b in range(n_col) if a or b], key=lambda at: -min(at[1], n_col - at[1])
    )

    def pair(sems, k):
        return (sems.at[k, 0], sems.at[k, 1])

    def ends(sems):
        return (sems.at[0], sems.at[1])

    parts = (t_ref, v_ref, g.part_one, g.part_two)
    loads = [pltpu.make_async_copy(ins[k], parts[k], g.loaded.at[k]) for k in range(4)]
    start_all(loads)
    barrier = pltpu.get_barrier_semaphore()
    for a, b in far:
        pl.semaphore_signal(barrier, inc=1, device_id=(row_peers[a], col_peers[b]), device_id_type=MESH)
    for copy in loads:
        copy.wait()
    contracted = right_product(v_ref[...], t_ref[...].reshape(rows_one * rows_two, depth))
    for tile in range(tiles):
        g.parted[pl.ds(tile, rank, stride=tiles), :] = contracted[:, tile * LANES : (tile + 1) * LANES]
    pl.semaphore_wait(barrier, n - 1)
    place = aligned((col * n_row + row) * SUBLANES, SUBLANES)
    start_all(
        [
            remote(
                g.parted.at[aligned((row_peers[a] * n_col + col_peers[b]) * SUBLANES, SUBLANES), :],
                g.held.at[place, :], ends(g.d_held), row_peers[a], col_peers[b],
            )
            for a, b in far
        ]
    )
    own_one, own_two = aligned(row * rows_one, rows_one), aligned(col * rows_two, rows_two)
    start_all([remote(g.part_two, g.all_two.at[own_two, :], ends(g.d_two), row, col_peers[d]) for d in range(1, n_col)])
    start_all([remote(g.part_one, g.all_one.at[own_one, :], ends(g.d_one), row_peers[d], col) for d in range(1, n_row)])

    def block_source(which, peer):
        return t_ref.at[
            :,
            aligned(peer // 2 * SUBLANES, SUBLANES),
            aligned(lax.rem(peer, 2) * half + which * LANES, LANES, LANES),
        ]

    def block_target(which):
        return g.block.at[which, pl.ds(row * rows_one, rows_one)]

    def block_start(which):
        start_all(
            [
                remote(block_source(which, row_peers[d]), block_target(which), ends(g.d_block), row_peers[d], col)
                for d in range(1, n_row)
            ]
        )

    block_start(0)
    start_all([pltpu.make_async_copy(block_source(w, row), block_target(w), g.kept.at[0]) for w in range(portions)])
    g.held[place, :] = g.parted[aligned(me * SUBLANES, SUBLANES), :]
    g.all_one[own_one, :] = g.part_one[...]
    g.all_two[own_two, :] = g.part_two[...]
    for end in range(2):
        wait_bytes(g.all_two.at[pl.ds(0, n_two - rows_two), :], g.d_two.at[end])
        wait_bytes(g.all_one.at[pl.ds(0, n_one - rows_one), :], g.d_one.at[end])
        wait_bytes(g.held.at[pl.ds(0, (n - 1) * SUBLANES), :], g.d_held.at[end])
    group = lane_groups(rows_two)
    for c in range(share):
        for tile in range(tiles):
            blocks = [
                g.held[pl.ds(q * n_row * SUBLANES + c * tiles + tile, n_row, stride=SUBLANES), :] for q in range(n_col)
            ]
            for s in range(n_col):
                line = shifted(blocks[0], -s * rows_two)
                for q in range(1, n_col):
                    line = jnp.where(group == q, shifted(blocks[q], (q - s) * rows_two), line)
                g.faces[pl.ds(c * n_one + tile * n_col + s, n_row, stride=rows_one), :] = line

    count = LANES // n_row
    own_rows = aligned(row * count, count)

    def gram_first(w):
        start_all(
            [
                remote(
                    g.gram_part.at[w, aligned(row_peers[d] * count, count), :], g.gram_parts.at[w, d],
                    pair(g.d_gram_row, w), row_peers[d], col,
                )
                for d in range(1, n_row)
            ]
        )

    def gram_second(w):
        wait_bytes(g.gram_parts.at[w, pl.ds(0, n_row - 1)], g.d_gram_row.at[w, 1])
        total = g.gram_part[w, own_rows, :]
        for d in range(1, n_row):
            total = total + g.gram_parts[w, d]
        g.gram_planes[w, col] = total
        start_all(
            [
                remote(g.gram_planes.at[w, col], g.gram_planes.at[w, col], pair(g.d_gram_col, w), row, col_peers[d])
                for d in range(1, n_col)
            ]
        )

    def gram_third(w):
        wait_bytes(g.gram_planes.at[w, pl.ds(0, n_col - 1)], g.d_gram_col.at[w, 1])
        total = g.gram_planes[w, 0]
        for q in range(1, n_col):
            total = total + g.gram_planes[w, q]
        g.gram_sum[w, own_rows, :] = total
        start_all(
            [
                remote(
                    g.gram_sum.at[w, own_rows, :], g.gram_sum.at[w, own_rows, :],
                    pair(g.d_gram_all, w), row_peers[d], col,
                )
                for d in range(1, n_row)
            ]
        )

    def gram_end(w):
        wait_bytes(g.gram_sum.at[w, pl.ds(0, LANES - count), :], g.d_gram_all.at[w, 1])
        wait_bytes(g.gram_parts.at[w, pl.ds(0, n_row - 1)], g.d_gram_row.at[w, 0])
        wait_bytes(g.gram_planes.at[w, pl.ds(0, n_col - 1)], g.d_gram_col.at[w, 0])
        wait_bytes(g.gram_sum.at[w, pl.ds(0, LANES - count), :], g.d_gram_all.at[w, 0])

    def self_gram(slabs):
        total = right_product(slabs[0], slabs[0])
        for slab in slabs[1:]:
            total = total + right_product(slab, slab)
        return total

    g.gram_part[0] = self_gram(
        [product(g.faces[c * n_one : (c + 1) * n_one, :], g.all_two[...]) for c in range(share)]
    )
    gram_first(0)
    for c in range(share):
        g.turned[c] = g.faces[c * n_one : (c + 1) * n_one, :].T
    g.basis_one[...] = g.all_one[...].T
    g.basis_two[...] = g.all_two[...].T
    gram_second(0)
    block_start(1)
    gram_third(0)
    gram_end(0)
    for which in range(2, portions):
        block_start(which)
    settle_turned(g.gram_sum.at[0], g.basis_one)
    basis_one = g.basis_one[...]

    g.gram_part[1] = self_gram([right_product(g.turned[c], basis_one) for c in range(share)])
    gram_first(1)
    g.factors[0] = basis_one * math.sqrt(n_one)
    for end in range(2):
        wait_bytes(g.block.at[:, pl.ds(0, n_one - rows_one)], g.d_block.at[end])
    wait_bytes(g.block.at[:, pl.ds(0, rows_one)], g.kept.at[0])
    flat_block = g.block.reshape(portions * n_one * SUBLANES, LANES)
    flat_mixed = g.mixed.reshape(portions * rank * SUBLANES, LANES)
    for s in range(SUBLANES):
        face = [flat_block[pl.ds(w * n_one * SUBLANES + s, n_one, stride=SUBLANES), :] for w in range(portions)]
        face = product(basis_one, jnp.concatenate(face, axis=1))
        for w in range(portions):
            flat_mixed[pl.ds(w * rank * SUBLANES + s, rank, stride=SUBLANES), :] = face[:, w * LANES : (w + 1) * LANES]
    gram_second(1)
    pieces = rank // n
    lines = aligned(col * rows_two + chip * SUBLANES, SUBLANES)
    parts = pl.ds(core * portions, portions)
    start_all(
        [
            remote(
                g.mixed.at[:, pl.ds((row_peers[a] * n_col + col_peers[b]) * pieces, pieces)], g.joined.at[parts, :, lines, :],
                ends(g.d_mixed), row_peers[a], col_peers[b],
            )
            for a, b in far
        ]
    )
    gram_third(1)
    g.joined[parts, :, lines, :] = g.mixed[:, pl.ds(me * pieces, pieces)]
    gram_end(1)
    settle_turned(g.gram_sum.at[1], g.basis_two)
    basis_two = g.basis_two[...]
    g.factors[1] = basis_two * math.sqrt(n_two)
    stores = [pltpu.make_async_copy(g.factors.at[k], outs[k], g.stored.at[k]) for k in range(2)]
    start_all(stores)
    for end in range(2):
        wait_bytes(g.mixed.at[:, pl.ds(0, rank - pieces)], g.d_mixed.at[end])
    for a in range(pieces):
        g.slab[a * rank : (a + 1) * rank, :] = product(
            basis_two, jnp.concatenate([g.joined[w, a] for w in range(2 * portions)], axis=1)
        )

    bands, chunk = depth // BAND, rank // n_row
    own_chunk = aligned(row * chunk, chunk)

    def band(ref, w):
        return ref[:, w * BAND : (w + 1) * BAND]

    def added(terms):
        total = terms[0]
        for term in terms[1:]:
            total = total + term
        return total

    def inner():
        return added([right_product(band(g.iterate, w), band(g.iterate, w)) for w in range(bands)])

    def one(step, carry):
        turn = lax.rem(step, 2)
        cross = g.cross[...]
        for w in range(bands):
            g.image_part[step, w] = product(cross, band(g.slab, w))
            start_all(
                [
                    remote(
                        g.image_part.at[step, w, aligned(row_peers[d] * chunk, chunk), :], g.image_parts.at[step, w, d],
                        pair(g.d_image_row, w), row_peers[d], col,
                    )
                    for d in range(1, n_row)
                ]
            )
        square = inner()
        for w in range(bands):
            wait_bytes(g.image_parts.at[step, w, pl.ds(0, n_row - 1)], g.d_image_row.at[w, 1])
            g.image_planes[step, w, col] = added(
                [g.image_part[step, w, own_chunk, :]] + [g.image_parts[step, w, d] for d in range(1, n_row)]
            )
            start_all(
                [
                    remote(
                        g.image_planes.at[step, w, col], g.image_planes.at[step, w, col],
                        pair(g.d_image_col.at[turn], w), row, col_peers[d],
                    )
                    for d in range(1, n_col)
                ]
            )
        inverse = jnp.where(step == 0, unit(rank), inverse_factor(square))
        g.linv[...] = inverse
        for w in range(bands):
            wait_bytes(g.image_planes.at[step, w, pl.ds(0, n_col - 1)], g.d_image_col.at[turn, w, 1])
            g.image[step, w, own_chunk, :] = added([g.image_planes[step, w, q] for q in range(n_col)])
            start_all(
                [
                    remote(
                        g.image.at[step, w, own_chunk, :], g.image.at[step, w, own_chunk, :],
                        pair(g.d_image_all, w), row_peers[d], col,
                    )
                    for d in range(1, n_row)
                ]
            )
        terms = []
        for w in range(bands):
            wait_bytes(g.image.at[step, w, pl.ds(0, rank - chunk), :], g.d_image_all.at[w, 1])
            now = product(g.linv[...], g.image[step, w])
            g.iterate[:, w * BAND : (w + 1) * BAND] = now
            terms.append(right_product(now, band(g.slab, w)))
        g.cross[...] = added(terms)
        for w in range(bands):
            wait_bytes(g.image_parts.at[step, w, pl.ds(0, n_row - 1)], g.d_image_row.at[w, 0])
            wait_bytes(g.image_planes.at[step, w, pl.ds(0, n_col - 1)], g.d_image_col.at[turn, w, 0])
            wait_bytes(g.image.at[step, w, pl.ds(0, rank - chunk), :], g.d_image_all.at[w, 0])
        return carry

    g.iterate[...] = v_ref[...]
    g.cross[...] = added([right_product(band(g.iterate, w), band(g.slab, w)) for w in range(bands)])
    lax.fori_loop(0, STEPS, one, 0)
    g.core_own[...] = g.cross[...].T.reshape(pieces, rank, rank)
    own_b = rank // n_col
    own_pieces = pl.ds(col * pieces, pieces)
    start_all(
        [
            remote(
                g.core_own.at[:, aligned(col_peers[d] * own_b, own_b), :], g.core_all.at[own_pieces],
                ends(g.d_core), row, col_peers[d],
            )
            for d in range(1, n_col)
        ]
    )
    stores.append(pltpu.make_async_copy(g.iterate, outs[2], g.stored.at[2]))
    stores[-1].start()
    g.core_all[own_pieces] = g.core_own[:, aligned(col * own_b, own_b), :]
    g.linv[...] = inverse_factor(inner())
    stores.append(pltpu.make_async_copy(g.linv, outs[3], g.stored.at[3]))
    stores[-1].start()
    for end in (1, 0):
        wait_bytes(g.core_all.at[pl.ds(0, (n_col - 1) * pieces)], g.d_core.at[end])
    stores.append(pltpu.make_async_copy(g.core_all, outs[4], g.stored.at[4]))
    stores[-1].start()
    for copy in stores:
        copy.wait()


def finish_kernel(one_ref, two_ref, last_ref, linv_ref, piece_ref, f1_ref, f2_ref, f3_ref, core_ref):
    f1_ref[...] = one_ref[...]
    f2_ref[...] = two_ref[...]
    linv = linv_ref[...]
    f3_ref[...] = product(linv, last_ref[...]) * math.sqrt(last_ref.shape[1])
    core_ref[...] = right_product(piece_ref[...].reshape(core_ref.shape), linv)


def shared(n_row, n_col, tensor, start_one, start_two, start_three):
    rows_one, rows_two, depth = tensor.shape
    rank = start_three.shape[1]
    own_a, own_b = rank // n_row, rank // n_col
    spec = pl.BlockSpec(memory_space=pltpu.VMEM)
    scratch = chain_scratch(n_row, n_col, rows_one, rows_two, depth, rank)

    def outs(*shapes):
        return [jax.ShapeDtypeStruct(shape, jnp.float32) for shape in shapes]

    chained = pl.pallas_call(
        functools.partial(chain_kernel, n_row, n_col, tuple(scratch)),
        out_shape=outs((rank, LANES), (rank, LANES), (rank, depth), (rank, rank), (own_a, own_b, rank)),
        in_specs=[pl.BlockSpec(memory_space=pltpu.HBM)] * 4,
        out_specs=[pl.BlockSpec(memory_space=pltpu.HBM)] * 5,
        scratch_shapes=list(scratch.values()),
        compiler_params=pltpu.CompilerParams(
            collective_id=1, has_side_effects=True, vmem_limit_bytes=67043328 - 300 * 1024
        ),
        cost_estimate=pl.CostEstimate(flops=10**9, bytes_accessed=10**7, transcendentals=0),
        name="chain",
    )(tensor, start_three.T, start_one, start_two)
    factor_one, factor_two, factor_three, core = pl.pallas_call(
        finish_kernel,
        out_shape=outs((rank, LANES), (rank, LANES), (rank, depth), (own_a * own_b, rank)),
        in_specs=[spec] * 5,
        out_specs=[spec] * 4,
        compiler_params=pltpu.CompilerParams(vmem_limit_bytes=67043328 - 100 * 1024),
        cost_estimate=pl.CostEstimate(flops=10**7, bytes_accessed=10**6, transcendentals=0),
        name="finish",
    )(*chained)
    return (factor_one.T, factor_two.T, factor_three.T, core.reshape(own_a, own_b, rank).transpose(2, 0, 1))


def solution(mesh):
    n_row, n_col = mesh.shape["row"], mesh.shape["col"]
    n = n_row * n_col

    def on_device(tensor, start_one, start_two, start_three):
        rows_one, rows_two, depth = tensor.shape
        rank = start_three.shape[1]
        plane, span = n_row // 2, rows_one * rows_two
        even = (
            n_row % 2 == 0
            and rows_one * n_row == rows_two * n_col == LANES
            and rows_two == plane * SUBLANES
            and rows_one % SUBLANES == 0
            and depth % BAND == 0
            and rank % (n_row * SUBLANES) == 0
            and rank % (n_col * SUBLANES) == 0
            and rank % n == 0
            and rank // n * (span // LANES) == SUBLANES
        )
        if even:
            return shared(n_row, n_col, tensor, start_one, start_two, start_three)
        return general(tensor, start_one, start_two, start_three)

    return jax.shard_map(
        on_device,
        mesh=mesh,
        in_specs=(P("row", "col", None), P("row", None), P("col", None), P()),
        out_specs=(P(), P(), P(), P(None, "row", "col")),
        check_vma=False,
    )
```

```python
import functools
import math
import types

import jax
import jax.numpy as jnp
from jax import lax
from jax.experimental import pallas as pl
from jax.experimental.pallas import tpu as pltpu
from jax.sharding import PartitionSpec as P

STEPS = 4


HIGHEST = lax.Precision.HIGHEST
MESH = pl.DeviceIdType.MESH
SUBLANES = 8
LANES = 128
BAND = 2 * LANES


def product(left, right):
    return jnp.dot(left, right, precision=HIGHEST, preferred_element_type=jnp.float32)


def left_product(left, right):
    return lax.dot_general(
        left, right, (((0,), (0,)), ((), ())), precision=HIGHEST, preferred_element_type=jnp.float32
    )


def right_product(left, right):
    return lax.dot_general(
        left, right, (((1,), (1,)), ((), ())), precision=HIGHEST, preferred_element_type=jnp.float32
    )


def cross_product(left, right):
    return lax.dot_general(
        left, right, (((0,), (1,)), ((), ())), precision=HIGHEST, preferred_element_type=jnp.float32
    )


def orthonormal(matrix, inner):
    lower = jnp.linalg.cholesky(inner)
    return jax.scipy.linalg.solve_triangular(lower, matrix.T, lower=True).T


def settle(gram_whole, basis):
    for iteration in range(STEPS):
        image = product(gram_whole, basis)
        basis = orthonormal(image, left_product(image, image))
    return basis


def general(tensor, start_one, start_two, start_three):
    rows_one, rows_two, depth = tensor.shape
    rank = start_three.shape[1]
    flat = tensor.reshape(rows_one * rows_two, depth)
    contracted = cross_product(start_three, flat).reshape(rank, rows_one, rows_two)
    part_one = jnp.einsum("cij,jb->ibc", contracted, start_two, precision=HIGHEST).reshape(
        rows_one, rank * rank
    )
    slab_one = lax.psum_scatter(part_one, "col", scatter_dimension=1, tiled=True)
    slab_rows_one = lax.all_gather(slab_one, "row", axis=0, tiled=True)
    gram_one = lax.psum(right_product(slab_rows_one, slab_rows_one), "col")
    basis_one = settle(gram_one, lax.all_gather(start_one, "row", axis=0, tiled=True))
    own_one = lax.dynamic_slice_in_dim(basis_one, lax.axis_index("row") * rows_one, rows_one, 0)
    part_two = jnp.einsum("cij,ia->jac", contracted, own_one, precision=HIGHEST).reshape(
        rows_two, rank * rank
    )
    slab_two = lax.psum_scatter(part_two, "row", scatter_dimension=1, tiled=True)
    slab_rows_two = lax.all_gather(slab_two, "col", axis=0, tiled=True)
    gram_two = lax.psum(right_product(slab_rows_two, slab_rows_two), "row")
    basis_two = settle(gram_two, lax.all_gather(start_two, "col", axis=0, tiled=True))
    own_two = lax.dynamic_slice_in_dim(basis_two, lax.axis_index("col") * rows_two, rows_two, 0)
    received = lax.all_to_all(tensor, "row", split_axis=2, concat_axis=0, tiled=True)
    count, items, cells = received.shape
    merged = left_product(basis_one, received.reshape(count, items * cells))
    mixed = merged.reshape(rank, items, cells)
    part_three = jnp.einsum("ajk,jb->kba", mixed, own_two, precision=HIGHEST)
    cells_here = part_three.shape[0]
    slab_three = lax.psum_scatter(
        part_three.reshape(cells_here, rank * rank), "col", scatter_dimension=1, tiled=True
    )
    gram_part_three = right_product(slab_three, lax.all_gather(slab_three, "row", axis=0, tiled=True))
    gram_three = lax.psum(gram_part_three, "col")
    basis_three = start_three
    own_three = start_three
    for iteration in range(STEPS):
        image = product(gram_three, basis_three)
        inner = lax.psum(left_product(image, image), "row")
        own_three = orthonormal(image, inner)
        basis_three = lax.all_gather(own_three, "row", axis=0, tiled=True)
    core_part = left_product(own_three, slab_three)
    core_part = core_part.reshape(rank, core_part.shape[1] // rank, rank)
    core = lax.psum_scatter(core_part, "row", scatter_dimension=2, tiled=True).transpose(0, 2, 1)
    factor_one = basis_one * math.sqrt(basis_one.shape[0])
    factor_two = basis_two * math.sqrt(basis_two.shape[0])
    factor_three = basis_three * math.sqrt(basis_three.shape[0])
    return (factor_one, factor_two, factor_three, core)


def unit(size):
    shape = (size, size)
    return (lax.broadcasted_iota(jnp.int32, shape, 0) == lax.broadcasted_iota(jnp.int32, shape, 1)).astype(jnp.float32)


def inverse_factor(inner):
    n = inner.shape[0]
    groups = n // SUBLANES
    whole = jnp.concatenate([inner, unit(n)], axis=1)
    shape = (SUBLANES, whole.shape[1])
    rows = [whole[g * SUBLANES : (g + 1) * SUBLANES] for g in range(groups)]
    sub = lax.broadcasted_iota(jnp.int32, shape, 0)
    zero = rows[0] * 0.0

    def across(value, t):
        return jnp.broadcast_to(value[t : t + 1, :], shape)

    def column(g, k):
        return jnp.broadcast_to(rows[g][:, k : k + 1], shape)

    diagonal = [column(0, k) + zero for k in range(SUBLANES)]
    out = []
    for base in range(groups):
        head = base * SUBLANES
        panel = [[column(g, head + k) for g in range(base + 1, groups)] for k in range(SUBLANES)]
        coming = []
        if base + 1 < groups:
            coming = [column(base + 1, head + SUBLANES + k) for k in range(SUBLANES)]
            panel[0][0] = panel[0][0] + zero
        held = None
        for t in range(SUBLANES):
            pivot = across(diagonal[t], t)
            held = pivot if held is None else jnp.where(sub >= t, pivot, held)
            scale = 1.0 / pivot
            row = across(rows[base], t)
            heads = [across(diagonal[s], t) for s in range(t + 1, SUBLANES)]
            factor = jnp.where(sub > t, diagonal[t] * scale, 0.0)
            for s in range(t + 1, SUBLANES):
                diagonal[s] = diagonal[s] - factor * heads[s - t - 1]
            rows[base] = rows[base] - factor * row
            for k, g in enumerate(range(base + 1, groups)):
                factor = panel[t][k] * scale
                if k == 0:
                    coming = [coming[s] - factor * across(panel[t][0], s) for s in range(SUBLANES)]
                rows[g] = rows[g] - factor * row
                for s in range(t + 1, SUBLANES):
                    panel[s][k] = panel[s][k] - factor * heads[s - t - 1]
        out.append(rows[base] * lax.rsqrt(held))
        diagonal = coming
    return jnp.concatenate(out, axis=0)[:, n:]


def lane_groups(width):
    return lax.div(lax.broadcasted_iota(jnp.int32, (1, LANES), 1), width)


def shifted(value, amount):
    amount = amount % LANES
    return value if amount == 0 else pltpu.roll(value, amount, 1)


def settle_turned(gram_ref, basis_ref):
    basis_ref[...] = product(basis_ref[...], gram_ref[...])

    def one(_, carry):
        image = basis_ref[...]
        further = product(image, gram_ref[...])
        basis_ref[...] = product(inverse_factor(right_product(image, image)), further)
        return carry

    lax.fori_loop(0, STEPS - 1, one, 0)
    image = basis_ref[...]
    basis_ref[...] = product(inverse_factor(right_product(image, image)), image)


def aligned(start, count, multiple=SUBLANES):
    return pl.ds(pl.multiple_of(start, multiple), count)


def remote(source, target, sems, row, col):
    return pltpu.make_async_remote_copy(
        src_ref=source, dst_ref=target, send_sem=sems[0], recv_sem=sems[1], device_id=(row, col), device_id_type=MESH
    )


def start_all(made):
    for copy in made:
        copy.start()


def wait_bytes(ref, sem):
    pltpu.make_async_copy(ref, ref, sem).wait()


def chain_scratch(n_row, n_col, rows_one, rows_two, depth, rank):
    n, half, n_one, n_two = n_row * n_col, depth // 2, LANES, LANES
    share, portions, pieces = rank // n, half // LANES, rank // n
    bands, chunk, own_b = depth // BAND, rank // n_row, rank // n_col

    def buffer(*shape):
        return pltpu.VMEM(shape, jnp.float32)

    def dma(*shape):
        return pltpu.SemaphoreType.DMA(shape)

    return dict(
        tensor=buffer(rows_one, rows_two, depth),
        start=buffer(rank, depth),
        part_one=buffer(rows_one, rank),
        part_two=buffer(rows_two, rank),
        parted=buffer(n * SUBLANES, LANES),
        held=buffer(n * SUBLANES, LANES),
        faces=buffer(share * n_one, n_two),
        turned=buffer(share, n_two, n_one),
        all_one=buffer(n_one, rank),
        all_two=buffer(n_two, rank),
        gram_part=buffer(2, LANES, LANES),
        gram_parts=buffer(2, n_row, LANES // n_row, LANES),
        gram_planes=buffer(2, n_col, LANES // n_row, LANES),
        gram_sum=buffer(2, LANES, LANES),
        basis_one=buffer(rank, n_one),
        basis_two=buffer(rank, n_two),
        factors=buffer(2, rank, LANES),
        block=buffer(portions, n_one, SUBLANES, LANES),
        mixed=buffer(portions, rank, SUBLANES, LANES),
        joined=buffer(2 * portions, pieces, n_two, LANES),
        slab=buffer(pieces, rank, depth),
        core_slab=buffer(n_col * pieces, own_b, depth),
        square=buffer(rank, rank),
        linv=buffer(rank, rank),
        iterate=buffer(rank, depth),
        cross=buffer(rank, pieces * rank),
        image=buffer(STEPS + 1, bands, rank, BAND),
        image_part=buffer(STEPS, bands, rank, BAND),
        image_parts=buffer(STEPS, bands, n_row, chunk, BAND),
        image_planes=buffer(STEPS, bands, n_col, chunk, BAND),
        core_all=buffer(n_col * pieces, own_b, rank),
        loaded=dma(4),
        stored=dma(5),
        d_held=dma(2),
        d_one=dma(2),
        d_two=dma(2),
        d_block=dma(2),
        kept=dma(1),
        d_gram_row=dma(2, 2),
        d_gram_col=dma(2, 2),
        d_gram_all=dma(2, 2),
        d_mixed=dma(2),
        d_image_row=dma(bands, 2),
        d_image_col=dma(2, bands, 2),
        d_image_all=dma(bands, 2),
        d_core=dma(2),
    )


def chain_kernel(n_row, n_col, names, *refs):
    ins, outs, refs = refs[:4], refs[4:9], refs[9:]
    g = types.SimpleNamespace(**dict(zip(names, refs)))
    t_ref, v_ref = g.tensor, g.start
    row, col = lax.axis_index("row"), lax.axis_index("col")
    n = n_row * n_col
    me, chip, core = row * n_col + col, row // 2, lax.rem(row, 2)
    rows_one, rows_two, depth = t_ref.shape
    rank, half = v_ref.shape[0], depth // 2
    share, tiles, portions = rank // n, rows_one * rows_two // LANES, half // LANES
    n_one = n_two = LANES
    row_peers = [lax.rem(row + d, n_row) for d in range(n_row)]
    col_peers = [lax.rem(col + d, n_col) for d in range(n_col)]
    far = sorted(
        [(a, b) for a in range(n_row) for b in range(n_col) if a or b], key=lambda at: -min(at[1], n_col - at[1])
    )

    def pair(sems, k):
        return (sems.at[k, 0], sems.at[k, 1])

    def ends(sems):
        return (sems.at[0], sems.at[1])

    parts = (t_ref, v_ref, g.part_one, g.part_two)
    loads = [pltpu.make_async_copy(ins[k], parts[k], g.loaded.at[k]) for k in range(4)]
    start_all(loads)
    barrier = pltpu.get_barrier_semaphore()
    for a, b in far:
        pl.semaphore_signal(barrier, inc=1, device_id=(row_peers[a], col_peers[b]), device_id_type=MESH)
    for copy in loads:
        copy.wait()
    contracted = right_product(v_ref[...], t_ref[...].reshape(rows_one * rows_two, depth))
    for tile in range(tiles):
        g.parted[pl.ds(tile, rank, stride=tiles), :] = contracted[:, tile * LANES : (tile + 1) * LANES]
    pl.semaphore_wait(barrier, n - 1)
    place = aligned((col * n_row + row) * SUBLANES, SUBLANES)
    start_all(
        [
            remote(
                g.parted.at[aligned((row_peers[a] * n_col + col_peers[b]) * SUBLANES, SUBLANES), :],
                g.held.at[place, :], ends(g.d_held), row_peers[a], col_peers[b],
            )
            for a, b in far
        ]
    )
    own_one, own_two = aligned(row * rows_one, rows_one), aligned(col * rows_two, rows_two)
    start_all([remote(g.part_two, g.all_two.at[own_two, :], ends(g.d_two), row, col_peers[d]) for d in range(1, n_col)])
    start_all([remote(g.part_one, g.all_one.at[own_one, :], ends(g.d_one), row_peers[d], col) for d in range(1, n_row)])

    def block_source(which, peer):
        return t_ref.at[
            :,
            aligned(peer // 2 * SUBLANES, SUBLANES),
            aligned(lax.rem(peer, 2) * half + which * LANES, LANES, LANES),
        ]

    def block_target(which):
        return g.block.at[which, pl.ds(row * rows_one, rows_one)]

    def block_start(which, peers):
        start_all(
            [
                remote(block_source(which, row_peers[d]), block_target(which), ends(g.d_block), row_peers[d], col)
                for d in peers
            ]
        )

    middle = n_row // 2
    block_start(0, range(1, n_row))
    start_all([pltpu.make_async_copy(block_source(w, row), block_target(w), g.kept.at[0]) for w in range(portions)])
    g.held[place, :] = g.parted[aligned(me * SUBLANES, SUBLANES), :]
    g.all_one[own_one, :] = g.part_one[...]
    g.all_two[own_two, :] = g.part_two[...]
    for end in range(2):
        wait_bytes(g.all_two.at[pl.ds(0, n_two - rows_two), :], g.d_two.at[end])
        wait_bytes(g.all_one.at[pl.ds(0, n_one - rows_one), :], g.d_one.at[end])
        wait_bytes(g.held.at[pl.ds(0, (n - 1) * SUBLANES), :], g.d_held.at[end])
    group = lane_groups(rows_two)
    for c in range(share):
        for tile in range(tiles):
            blocks = [
                g.held[pl.ds(q * n_row * SUBLANES + c * tiles + tile, n_row, stride=SUBLANES), :] for q in range(n_col)
            ]
            for s in range(n_col):
                line = shifted(blocks[0], -s * rows_two)
                for q in range(1, n_col):
                    line = jnp.where(group == q, shifted(blocks[q], (q - s) * rows_two), line)
                g.faces[pl.ds(c * n_one + tile * n_col + s, n_row, stride=rows_one), :] = line

    count = LANES // n_row
    own_rows = aligned(row * count, count)

    def gram_first(w):
        start_all(
            [
                remote(
                    g.gram_part.at[w, aligned(row_peers[d] * count, count), :], g.gram_parts.at[w, d],
                    pair(g.d_gram_row, w), row_peers[d], col,
                )
                for d in range(1, n_row)
            ]
        )

    def gram_second(w):
        wait_bytes(g.gram_parts.at[w, pl.ds(0, n_row - 1)], g.d_gram_row.at[w, 1])
        total = g.gram_part[w, own_rows, :]
        for d in range(1, n_row):
            total = total + g.gram_parts[w, d]
        g.gram_planes[w, col] = total
        start_all(
            [
                remote(g.gram_planes.at[w, col], g.gram_planes.at[w, col], pair(g.d_gram_col, w), row, col_peers[d])
                for d in range(1, n_col)
            ]
        )

    def gram_third(w):
        wait_bytes(g.gram_planes.at[w, pl.ds(0, n_col - 1)], g.d_gram_col.at[w, 1])
        total = g.gram_planes[w, 0]
        for q in range(1, n_col):
            total = total + g.gram_planes[w, q]
        g.gram_sum[w, own_rows, :] = total
        start_all(
            [
                remote(
                    g.gram_sum.at[w, own_rows, :], g.gram_sum.at[w, own_rows, :],
                    pair(g.d_gram_all, w), row_peers[d], col,
                )
                for d in range(1, n_row)
            ]
        )

    def gram_end(w):
        wait_bytes(g.gram_sum.at[w, pl.ds(0, LANES - count), :], g.d_gram_all.at[w, 1])
        wait_bytes(g.gram_parts.at[w, pl.ds(0, n_row - 1)], g.d_gram_row.at[w, 0])
        wait_bytes(g.gram_planes.at[w, pl.ds(0, n_col - 1)], g.d_gram_col.at[w, 0])
        wait_bytes(g.gram_sum.at[w, pl.ds(0, LANES - count), :], g.d_gram_all.at[w, 0])

    def self_gram(slabs):
        total = right_product(slabs[0], slabs[0])
        for slab in slabs[1:]:
            total = total + right_product(slab, slab)
        return total

    g.gram_part[0] = self_gram(
        [product(g.faces[c * n_one : (c + 1) * n_one, :], g.all_two[...]) for c in range(share)]
    )
    gram_first(0)
    block_start(1, range(1, middle))
    for c in range(share):
        g.turned[c] = g.faces[c * n_one : (c + 1) * n_one, :].T
    g.basis_one[...] = g.all_one[...].T
    g.basis_two[...] = g.all_two[...].T
    gram_second(0)
    block_start(1, range(middle, n_row))
    gram_third(0)
    for which in range(2, portions):
        block_start(which, range(1, n_row))
    gram_end(0)
    settle_turned(g.gram_sum.at[0], g.basis_one)
    basis_one = g.basis_one[...]

    g.gram_part[1] = self_gram([right_product(g.turned[c], basis_one) for c in range(share)])
    gram_first(1)
    g.factors[0] = basis_one * math.sqrt(n_one)
    for end in range(2):
        wait_bytes(g.block.at[:, pl.ds(0, n_one - rows_one)], g.d_block.at[end])
    wait_bytes(g.block.at[:, pl.ds(0, rows_one)], g.kept.at[0])
    flat_block = g.block.reshape(portions * n_one * SUBLANES, LANES)
    flat_mixed = g.mixed.reshape(portions * rank * SUBLANES, LANES)
    for s in range(SUBLANES):
        face = [flat_block[pl.ds(w * n_one * SUBLANES + s, n_one, stride=SUBLANES), :] for w in range(portions)]
        face = product(basis_one, jnp.concatenate(face, axis=1))
        for w in range(portions):
            flat_mixed[pl.ds(w * rank * SUBLANES + s, rank, stride=SUBLANES), :] = face[:, w * LANES : (w + 1) * LANES]
    pieces = rank // n
    lines = aligned(col * rows_two + chip * SUBLANES, SUBLANES)
    parts = pl.ds(core * portions, portions)

    def mixed_start(peers):
        start_all(
            [
                remote(
                    g.mixed.at[:, pl.ds((row_peers[a] * n_col + col_peers[b]) * pieces, pieces)],
                    g.joined.at[parts, :, lines, :], ends(g.d_mixed), row_peers[a], col_peers[b],
                )
                for a, b in peers
            ]
        )

    across = [at for at in far if at[1]]
    fifth = len(across) // 5
    mixed_start(across[:fifth])
    gram_second(1)
    mixed_start(across[fifth : 2 * fifth])
    gram_third(1)
    mixed_start(across[2 * fifth :] + [at for at in far if not at[1]])
    g.joined[parts, :, lines, :] = g.mixed[:, pl.ds(me * pieces, pieces)]
    gram_end(1)
    settle_turned(g.gram_sum.at[1], g.basis_two)
    basis_two = g.basis_two[...]
    g.factors[1] = basis_two * math.sqrt(n_two)
    stores = [pltpu.make_async_copy(g.factors.at[k], outs[k], g.stored.at[k]) for k in range(2)]
    start_all(stores)
    for end in range(2):
        wait_bytes(g.mixed.at[:, pl.ds(0, rank - pieces)], g.d_mixed.at[end])
    for a in range(pieces):
        g.slab[a] = product(
            basis_two, jnp.concatenate([g.joined[w, a] for w in range(2 * portions)], axis=1)
        )

    bands, chunk = depth // BAND, rank // n_row
    own_chunk = aligned(row * chunk, chunk)

    def band(w):
        return slice(w * BAND, (w + 1) * BAND)

    def slab(w):
        return g.slab[:, :, band(w)].reshape(pieces * rank, BAND)

    def added(terms):
        total = terms[0]
        for term in terms[1:]:
            total = total + term
        return total

    def scale(step):
        for w in range(bands):
            g.iterate[:, band(w)] = product(g.linv[...], g.image[step, w])
        return added([right_product(g.iterate[:, band(w)], g.iterate[:, band(w)]) for w in range(bands)])

    own_b = rank // n_col
    own_pieces = pl.ds(col * pieces, pieces)

    def one(step, carry):
        turn = lax.rem(step, 2)
        cross = g.cross[...]
        for w in range(bands):
            g.image_part[step, w] = product(cross, slab(w))
            start_all(
                [
                    remote(
                        g.image_part.at[step, w, aligned(row_peers[d] * chunk, chunk), :], g.image_parts.at[step, w, d],
                        pair(g.d_image_row, w), row_peers[d], col,
                    )
                    for d in range(1, n_row)
                ]
            )
        g.square[...] = scale(step)
        for w in range(bands):
            wait_bytes(g.image_parts.at[step, w, pl.ds(0, n_row - 1)], g.d_image_row.at[w, 1])
            g.image_planes[step, w, col] = added(
                [g.image_part[step, w, own_chunk, :]] + [g.image_parts[step, w, d] for d in range(1, n_row)]
            )
            start_all(
                [
                    remote(
                        g.image_planes.at[step, w, col], g.image_planes.at[step, w, col],
                        pair(g.d_image_col.at[turn], w), row, col_peers[d],
                    )
                    for d in range(1, n_col)
                ]
            )

        @pl.when(step > 0)
        def _():
            g.linv[...] = inverse_factor(g.square[...])

        for w in range(bands):
            wait_bytes(g.image_planes.at[step, w, pl.ds(0, n_col - 1)], g.d_image_col.at[turn, w, 1])
            g.image[step + 1, w, own_chunk, :] = added([g.image_planes[step, w, q] for q in range(n_col)])
            start_all(
                [
                    remote(
                        g.image.at[step + 1, w, own_chunk, :], g.image.at[step + 1, w, own_chunk, :],
                        pair(g.d_image_all, w), row_peers[d], col,
                    )
                    for d in range(1, n_row)
                ]
            )

        @pl.when(step < bands)
        def _():
            lanes = aligned(step * BAND, BAND, LANES)
            start_all(
                [
                    remote(
                        g.slab.at[:, aligned(col_peers[d] * own_b, own_b), lanes], g.core_slab.at[own_pieces, :, lanes],
                        ends(g.d_core), row, col_peers[d],
                    )
                    for d in range(1, n_col)
                ]
            )

        terms = []
        for w in range(bands):
            wait_bytes(g.image.at[step + 1, w, pl.ds(0, rank - chunk), :], g.d_image_all.at[w, 1])
            terms.append(right_product(g.image[step + 1, w], slab(w)))
        g.cross[...] = product(g.linv[...], added(terms))
        for w in range(bands):
            wait_bytes(g.image_parts.at[step, w, pl.ds(0, n_row - 1)], g.d_image_row.at[w, 0])
            wait_bytes(g.image_planes.at[step, w, pl.ds(0, n_col - 1)], g.d_image_col.at[turn, w, 0])
            wait_bytes(g.image.at[step + 1, w, pl.ds(0, rank - chunk), :], g.d_image_all.at[w, 0])
        return carry

    for w in range(bands):
        g.image[0, w] = v_ref[:, band(w)]
    g.linv[...] = unit(rank)
    g.core_slab[own_pieces] = g.slab[:, aligned(col * own_b, own_b), :]
    g.cross[...] = added([right_product(g.image[0, w], slab(w)) for w in range(bands)])
    lax.fori_loop(0, STEPS, one, 0)
    square = scale(STEPS)
    stores.append(pltpu.make_async_copy(g.iterate, outs[2], g.stored.at[2]))
    stores[-1].start()
    for end in (1, 0):
        wait_bytes(g.core_slab.at[pl.ds(0, (n_col - 1) * pieces)], g.d_core.at[end])
    whole = g.core_slab[...].reshape(n_col * pieces * own_b, depth)
    g.core_all[...] = right_product(whole, g.iterate[...]).reshape(g.core_all.shape)
    stores.append(pltpu.make_async_copy(g.core_all, outs[4], g.stored.at[4]))
    stores[-1].start()
    g.linv[...] = inverse_factor(square)
    stores.append(pltpu.make_async_copy(g.linv, outs[3], g.stored.at[3]))
    stores[-1].start()
    for copy in stores:
        copy.wait()


def finish_kernel(one_ref, two_ref, last_ref, linv_ref, piece_ref, f1_ref, f2_ref, f3_ref, core_ref):
    f1_ref[...] = one_ref[...]
    f2_ref[...] = two_ref[...]
    linv = linv_ref[...]
    f3_ref[...] = product(linv, last_ref[...]) * math.sqrt(last_ref.shape[1])
    core_ref[...] = right_product(piece_ref[...].reshape(core_ref.shape), linv)


def shared(n_row, n_col, tensor, start_one, start_two, start_three):
    rows_one, rows_two, depth = tensor.shape
    rank = start_three.shape[1]
    own_a, own_b = rank // n_row, rank // n_col
    spec = pl.BlockSpec(memory_space=pltpu.VMEM)
    scratch = chain_scratch(n_row, n_col, rows_one, rows_two, depth, rank)

    def outs(*shapes):
        return [jax.ShapeDtypeStruct(shape, jnp.float32) for shape in shapes]

    chained = pl.pallas_call(
        functools.partial(chain_kernel, n_row, n_col, tuple(scratch)),
        out_shape=outs((rank, LANES), (rank, LANES), (rank, depth), (rank, rank), (own_a, own_b, rank)),
        in_specs=[pl.BlockSpec(memory_space=pltpu.HBM)] * 4,
        out_specs=[pl.BlockSpec(memory_space=pltpu.HBM)] * 5,
        scratch_shapes=list(scratch.values()),
        compiler_params=pltpu.CompilerParams(
            collective_id=1, has_side_effects=True, vmem_limit_bytes=67043328 - 300 * 1024
        ),
        cost_estimate=pl.CostEstimate(flops=10**9, bytes_accessed=10**7, transcendentals=0),
        name="chain",
    )(tensor, start_three.T, start_one, start_two)
    factor_one, factor_two, factor_three, core = pl.pallas_call(
        finish_kernel,
        out_shape=outs((rank, LANES), (rank, LANES), (rank, depth), (own_a * own_b, rank)),
        in_specs=[spec] * 5,
        out_specs=[spec] * 4,
        compiler_params=pltpu.CompilerParams(vmem_limit_bytes=67043328 - 100 * 1024),
        cost_estimate=pl.CostEstimate(flops=10**7, bytes_accessed=10**6, transcendentals=0),
        name="finish",
    )(*chained)
    return (factor_one.T, factor_two.T, factor_three.T, core.reshape(own_a, own_b, rank).transpose(2, 0, 1))


def solution(mesh):
    n_row, n_col = mesh.shape["row"], mesh.shape["col"]
    n = n_row * n_col

    def on_device(tensor, start_one, start_two, start_three):
        rows_one, rows_two, depth = tensor.shape
        rank = start_three.shape[1]
        plane, span = n_row // 2, rows_one * rows_two
        even = (
            n_row % 2 == 0
            and rows_one * n_row == rows_two * n_col == LANES
            and rows_two == plane * SUBLANES
            and rows_one % SUBLANES == 0
            and depth % BAND == 0
            and depth // BAND <= STEPS
            and rank % (n_row * SUBLANES) == 0
            and rank % (n_col * SUBLANES) == 0
            and rank % n == 0
            and rank // n * (span // LANES) == SUBLANES
        )
        if even:
            return shared(n_row, n_col, tensor, start_one, start_two, start_three)
        return general(tensor, start_one, start_two, start_three)

    return jax.shard_map(
        on_device,
        mesh=mesh,
        in_specs=(P("row", "col", None), P("row", None), P("col", None), P()),
        out_specs=(P(), P(), P(), P(None, "row", "col")),
        check_vma=False,
    )
```
